32 devices in a mesh: grp: 2 (over x), pix: 16 (over z, y, core).
Axes of the slice: x: 2, y: 2, z: 4, core: 2. Of those that a mesh axis runs over, the one named last changes fastest.
Arguments:
- slcs: bfloat16 [2, 2048, 2048], P(None, ('grp', 'pix')), parts along dimension 1, may hold values from -6 to 6
- ref_date: int32 [2], P('grp'), parts along dimension 0, may hold values from 0 to 15
Outputs:
- spectrum: float32 [2, 2048, 2048], P(None, ('grp', 'pix')), parts along dimension 1
- compressed: float32 [2, 64, 4096], P(None, None, ('grp', 'pix')), parts along dimension 2
The draws below stay inside these ranges and needn't reach their ends.
There are 2 independent parts, one for each index of `grp`. The reference program is written for one: setup_inputs(seed, part) draws one part's arguments, and reference() takes and returns one part's arrays. A program takes and returns all parts, laid end to end along the dimension named above; each array names one. Nothing has to cross between parts.
All inputs are finite; a program needn't handle non-finite values.
Results may differ from the reference program's by a relative error of at most 0.0057.
Values may be sent and summed in bfloat16 or wider, within the bound.
A program may use at most 64 MiB of HBM per device.

```python
import math
import jax
import jax.numpy as jnp
from jax import lax

DATES = 16
ROWS = 64
COLS_DEV = 128
HALF_X = 5
HALF_Y = 2
POWER_ITERS = 6
COLS = 2048
N_PIX = 16


def shard_levels(key, shape, split, smallest, top_value):
    def one(dim, parts):
        draws = jax.random.uniform(jax.random.fold_in(jax.random.fold_in(key, 6), dim), (parts,), jnp.float32, smallest / len(split), top_value / len(split))
        return jnp.repeat(jnp.exp(draws), shape[dim] // parts).reshape((-1,) + (1,) * (len(shape) - dim - 1))

    level = one(*split[0])
    for cut in split[1:]:
        level = level * one(*cut)
    return level


def normal_values(stream_key, shape, deviation, limit, shards=(), kind=jnp.bfloat16):
    entries = deviation * jax.random.normal(stream_key, shape, jnp.float32)
    if shards:
        entries = entries * shard_levels(stream_key, shape, shards, -0.22, 0.18)
    return jnp.clip(entries, -limit, limit).astype(kind)


def setup_inputs(seed: int = 0, part: int = 0) -> dict:
    seeds = jax.random.split(jax.random.key(seed), 3)
    part_keys = jax.random.split(jax.random.fold_in(seeds[2], part), 3)
    return {
        "slcs": normal_values(part_keys[0], (2, DATES * ROWS, COLS), 1.0, 6.0, ((1, 16),)),
        "ref_date": jax.random.randint(part_keys[1], (1,), 0, DATES).astype(jnp.int32),
    }


LOADING = 0.25

def window_counts(line_count, column_count, first_column, strip_columns, half_lines, half_columns):
    line_index = jnp.arange(line_count, dtype=jnp.int32)
    column_index = first_column + jnp.arange(column_count, dtype=jnp.int32)
    line_span = jnp.minimum(line_index + half_lines, line_count - 1) - jnp.maximum(line_index - half_lines, 0) + 1
    column_span = jnp.minimum(column_index + half_columns, strip_columns - 1) - jnp.maximum(column_index - half_columns, 0) + 1
    return line_span.astype(jnp.float32)[:, None] * column_span.astype(jnp.float32)[None, :]

def box_window(products, column_count, half_lines, half_columns):
    summed = products[..., 0:column_count]
    for offset in range(1, 2 * half_columns + 1):
        summed = summed + products[..., offset:offset + column_count]
    line_count = summed.shape[-2]
    widths = [(0, 0)] * (summed.ndim - 2) + [(half_lines, half_lines), (0, 0)]
    padded = jnp.pad(summed, widths)
    result = padded[..., 0:line_count, :]
    for offset in range(1, 2 * half_lines + 1):
        result = result + padded[..., offset:offset + line_count, :]
    return result

def tile_covariance(window_data, counts, column_count):
    real_part = window_data[0]
    imag_part = window_data[1]

    def one_date(date_index):
        real_one = lax.dynamic_index_in_dim(real_part, date_index, 0, keepdims=True)
        imag_one = lax.dynamic_index_in_dim(imag_part, date_index, 0, keepdims=True)
        product_real = real_one * real_part + imag_one * imag_part
        product_imag = imag_one * real_part - real_one * imag_part
        stacked = jnp.stack([product_real, product_imag])
        return (box_window(stacked, column_count, HALF_Y, HALF_X) / counts).astype(jnp.bfloat16)
    return lax.map(one_date, jnp.arange(real_part.shape[0], dtype=jnp.int32))

def dct_table(line_count):
    frequency = jnp.arange(line_count, dtype=jnp.float32)[:, None]
    position = jnp.arange(line_count, dtype=jnp.float32)[None, :]
    weight = jnp.where(frequency == 0, math.sqrt(1.0 / line_count), math.sqrt(2.0 / line_count))
    return weight * jnp.cos(jnp.pi * (2.0 * position + 1.0) * frequency / (2.0 * line_count))

def process_tile(window_bf16, first_column, strip_columns, reference_date):
    window_data = window_bf16.astype(jnp.float32)
    column_count = window_data.shape[3] - 2 * HALF_X
    line_count = window_data.shape[2]
    counts = window_counts(line_count, column_count, first_column, strip_columns, HALF_Y, HALF_X)
    covariance = tile_covariance(window_data, counts, column_count)
    date_count = covariance.shape[0]
    pick = (jnp.arange(date_count, dtype=jnp.int32) == reference_date).astype(jnp.float32)[:, None, None]
    start_real = jnp.broadcast_to(pick, (date_count, line_count, column_count))
    start_imag = jnp.zeros_like(start_real)

    def power_step(step_index, vector):
        vec_real, vec_imag = vector
        cov_real = covariance[:, 0].astype(jnp.float32)
        cov_imag = covariance[:, 1].astype(jnp.float32)
        new_real = lax.optimization_barrier(jnp.sum(cov_real * vec_real[None] - cov_imag * vec_imag[None], axis=1)) + LOADING * vec_real
        new_imag = lax.optimization_barrier(jnp.sum(cov_real * vec_imag[None] + cov_imag * vec_real[None], axis=1)) + LOADING * vec_imag
        length = jnp.sqrt(lax.optimization_barrier(jnp.sum(new_real * new_real + new_imag * new_imag, axis=0)))
        return (new_real / length, new_imag / length)
    vec_real, vec_imag = lax.fori_loop(0, POWER_ITERS, power_step, (start_real, start_imag))
    ref_real = lax.optimization_barrier(jnp.sum(vec_real * pick, axis=0))
    ref_imag = lax.optimization_barrier(jnp.sum(vec_imag * pick, axis=0))
    linked_real = DATES * (vec_real * ref_real + vec_imag * ref_imag)
    linked_imag = DATES * (vec_imag * ref_real - vec_real * ref_imag)
    center = window_data[..., HALF_X:HALF_X + column_count]
    scaling = 1.0 / math.sqrt(DATES)
    comp_real = lax.optimization_barrier(jnp.sum(linked_real * center[0] + linked_imag * center[1], axis=0)) * scaling
    comp_imag = lax.optimization_barrier(jnp.sum(linked_real * center[1] - linked_imag * center[0], axis=0)) * scaling
    linked_stack = jnp.stack([linked_real, linked_imag])
    table = dct_table(line_count)
    transformed = jnp.einsum('qr,pkrc->pkqc', table, linked_stack, precision=lax.Precision.HIGHEST)
    spectrum_tile = transformed.reshape(2, date_count * line_count, column_count)
    return (spectrum_tile, jnp.stack([comp_real, comp_imag]))

def reference(slcs, ref_date):
    stacked_data = slcs.reshape(2, DATES, ROWS, COLS)
    padded = jnp.pad(stacked_data, ((0, 0), (0, 0), (0, 0), (HALF_X, HALF_X)))

    def one_tile(tile_index):
        first_column = (tile_index * COLS_DEV).astype(jnp.int32)
        window_bf16 = lax.dynamic_slice_in_dim(padded, first_column, COLS_DEV + 2 * HALF_X, 3)
        return process_tile(window_bf16, first_column, COLS, ref_date[0])
    spectra, compressed_tiles = lax.map(one_tile, jnp.arange(N_PIX, dtype=jnp.int32))
    spectrum = jnp.transpose(spectra, (1, 2, 0, 3)).reshape(2, DATES * ROWS, COLS)
    compressed = jnp.transpose(compressed_tiles, (1, 2, 0, 3)).reshape(2, ROWS, COLS)
    return (spectrum, compressed)
```

```python
import functools
import math

import jax
import jax.numpy as jnp
import numpy as np
from jax import lax
from jax.experimental import pallas as pl
from jax.experimental.pallas import tpu as pltpu
from jax.sharding import PartitionSpec as P

DATES = 16
ROWS = 64
HALF_X = 5
HALF_Y = 2
POWER_ITERS = 6
LOADING = 0.25

LANES = 128
SUB = 8
GROUPS = ROWS // SUB
HALO = 16
PACK = LANES // HALO
CHUNK = 4
SPAN = 8
TURN = 2
TURNS = GROUPS // TURN
SCALE = 2.0 ** -6
MESH = pl.DeviceIdType.MESH


def window_weights(columns):
    target = np.arange(columns)[None, :]
    band = np.abs(np.arange(columns)[:, None] - target) <= HALF_X
    outside = np.concatenate([np.arange(-HALF_X, 0), columns + np.arange(HALF_X)])
    halo = np.zeros((HALO, columns), np.float32)
    halo[: 2 * HALF_X] = np.abs(outside[:, None] - target) <= HALF_X
    both = np.concatenate([band.astype(np.float32), np.tile(halo, (PACK, 1))], axis=0)
    return jnp.asarray(both * SCALE, jnp.bfloat16)


def pick_weights(columns):
    pick = np.zeros((HALO, 2 * columns), np.float32)
    for h in range(HALF_X):
        pick[h, columns - HALF_X + h] = 1.0
        pick[HALF_X + h, columns + h] = 1.0
    return jnp.asarray(pick, jnp.bfloat16)


def order_weights(local_rows):
    per_date = ROWS // local_rows
    order = np.zeros((2, GROUPS, SUB, per_date, LANES), np.float32)
    for c in range(2):
        for line in range(ROWS):
            q, r = divmod(line, local_rows)
            order[c, line % GROUPS, line // GROUPS, q, c * local_rows + r] = 1.0
    return jnp.asarray(order.reshape(2 * ROWS, per_date * LANES), jnp.bfloat16)


def spread_weights():
    lane = np.arange(LANES)
    spread = (lane[:, None] % HALO) == (lane[None, :] % HALO)
    block = np.arange(PACK)[:, None, None] == (lane // HALO)[None, None, :]
    mask = np.broadcast_to(block, (PACK, 2 * SUB, LANES))
    return jnp.asarray(spread, jnp.bfloat16), jnp.asarray(mask, jnp.bfloat16)


def dct_weights(local_rows):
    frequency = np.arange(ROWS, dtype=np.float64)[:, None]
    position = np.arange(ROWS, dtype=np.float64)[None, :]
    weight = np.where(frequency == 0, math.sqrt(1.0 / ROWS), math.sqrt(2.0 / ROWS))
    table = weight * np.cos(np.pi * (2.0 * position + 1.0) * frequency / (2.0 * ROWS))
    table = table.reshape(ROWS // local_rows, local_rows, SUB, GROUPS).transpose(0, 1, 3, 2)
    big = np.zeros((ROWS // local_rows, 2, local_rows, GROUPS, 2, SUB), np.float32)
    for c in range(2):
        big[:, c, :, :, c] = table
    big = big.reshape(ROWS // local_rows, 2 * local_rows, 2 * ROWS)
    high = big.astype(jnp.bfloat16)
    low = (big - high.astype(np.float32)).astype(jnp.bfloat16)
    return jnp.asarray(np.concatenate([high, low], axis=2))


def pair_products(one, two):
    real = one[0] * two[0] + one[1] * two[1]
    imag = one[1] * two[0] - one[0] * two[1]
    return real, imag


def flips(a, size):
    out, bit = [], 1
    while bit < size:
        out.append(bit - 2 * bit * ((a // bit) % 2))
        bit *= 2
    return out


def flipped(a, deltas, b):
    for n, delta in enumerate(deltas):
        if isinstance(b, int):
            a = a + delta if (b >> n) & 1 else a
        else:
            a = a + delta * ((b // (1 << n)) % 2)
    return a


def link_kernel(devices, ref_ref, x_ref, both_ref, pick_ref, order_ref, spread_ref, mask_ref,
                o_ref, comp_ref,
                xs, win, hsend, hwin, hall, edge, wide, both, pick, order, spread, mask,
                stage, zb, summed, load, cov, vec, tile,
                local, ssem, rsem, hs, hr, ts, tr):
    columns = win.shape[3]
    local_rows = win.shape[2]
    strip_columns = x_ref.shape[2]
    per_date = ROWS // local_rows
    me = lax.axis_index("pix")
    my_date = me // per_date
    turns = flips(me, devices)
    date_turns = turns[(per_date - 1).bit_length():]
    peers = [flipped(me, turns, off) for off in range(devices)]
    bf16, f32 = jnp.bfloat16, jnp.float32

    loads = [
        pltpu.make_async_copy(src, dst, local.at[n])
        for n, (src, dst) in enumerate((
            (x_ref, xs.at[:, :, columns:columns + strip_columns]),
            (both_ref, both), (pick_ref, pick), (order_ref, order), (spread_ref, spread),
            (mask_ref, mask),
        ))
    ]
    for copy in loads:
        copy.start()
    barrier = pltpu.get_barrier_semaphore()
    for peer in peers[1:]:
        pl.semaphore_signal(barrier, inc=1, device_id={"pix": peer}, device_id_type=MESH)

    margin = jnp.zeros((2, local_rows, columns), bf16)
    xs[:, :, 0:columns] = margin
    xs[:, :, columns + strip_columns:2 * columns + strip_columns] = margin

    first_column = me * columns
    sub = lax.broadcasted_iota(jnp.int32, (SUB, columns), 0)
    lane = lax.broadcasted_iota(jnp.int32, (SUB, columns), 1) + first_column
    across = jnp.minimum(lane + HALF_X, strip_columns - 1) - jnp.maximum(lane - HALF_X, 0) + 1
    for g in range(GROUPS):
        line = sub * GROUPS + g
        along = jnp.minimum(line + HALF_Y, ROWS - 1) - jnp.maximum(line - HALF_Y, 0) + 1
        load[g] = (along * across).astype(f32) * (LOADING * SCALE)

    for copy in loads:
        copy.wait()

    blocks = 4
    def cut_halos(n, carry):
        for q in range(blocks):
            at = (n * blocks + q) * columns
            left = xs[:, :, pl.ds(pl.multiple_of(at, columns), columns)]
            right = xs[:, :, pl.ds(pl.multiple_of(at + 2 * columns, columns), columns)]
            near = jnp.concatenate(
                [left.reshape(2 * local_rows, columns), right.reshape(2 * local_rows, columns)], axis=1
            )
            if 2 * local_rows < LANES:
                fill = jnp.zeros((LANES - 2 * local_rows, 2 * columns), bf16)
                near = jnp.concatenate([near, fill], axis=0)
            got = lax.dot_general(
                pick[...], near, (((1,), (1,)), ((), ())), preferred_element_type=f32
            )
            hsend[n * blocks + q] = got.astype(bf16)
        return carry

    lax.fori_loop(0, devices // blocks, cut_halos, 0)

    pl.semaphore_wait(barrier, devices - 1)

    def block(n):
        return xs.at[:, :, pl.ds(pl.multiple_of((n + 1) * columns, columns), columns)]

    def main_copy(off, peer):
        return pltpu.make_async_remote_copy(
            src_ref=block(peer), dst_ref=win.at[me], send_sem=ssem.at[off], recv_sem=rsem.at[off],
            device_id={"pix": peer}, device_id_type=MESH,
        )

    def halo_copy(off, peer):
        return pltpu.make_async_remote_copy(
            src_ref=hsend.at[peer], dst_ref=hwin.at[me], send_sem=hs.at[off],
            recv_sem=hr.at[off], device_id={"pix": peer}, device_id_type=MESH,
        )

    halos = [halo_copy(off, peers[off]) for off in range(1, devices)]
    mains = [main_copy(off, peers[off]) for off in range(1, devices)]
    for c in halos + mains:
        c.start()
    own = [
        pltpu.make_async_copy(block(me), win.at[me], local.at[6]),
        pltpu.make_async_copy(hsend.at[me], hwin.at[me], local.at[7]),
    ]
    for c in own:
        c.start()
    for c in own + halos:
        c.wait()

    def date_at(p):
        return flipped(my_date, date_turns, p)

    for p in range(DATES):
        for q in range(per_date):
            hall[p * HALO:(p + 1) * HALO, q * LANES:(q + 1) * LANES] = hwin[date_at(p) * per_date + q]
    got = lax.dot_general(
        order[...], hall[...], (((1,), (1,)), ((), ())), preferred_element_type=f32
    ).astype(bf16)
    for half in range(DATES // PACK):
        edge[half] = got[:, half * LANES:(half + 1) * LANES].reshape(2, ROWS, LANES)

    def tall(value):
        return jnp.concatenate([value] * (ROWS // (2 * SUB)), axis=0)

    def spread_halos(p, carry):
        part = edge[p // PACK]
        keep = tall(mask[p % PACK])
        kept = jnp.concatenate([part[0] * keep, part[1] * keep], axis=0)
        got = jnp.dot(kept, spread[...], preferred_element_type=f32)
        wide[p] = got.astype(bf16).reshape(2, ROWS, LANES)
        return carry

    lax.fori_loop(0, DATES, spread_halos, 0)

    def window_sums(plane):
        rows = [plane[g * SUB:(g + 1) * SUB] for g in range(GROUPS)]
        before = [jnp.where(sub == 0, 0.0, pltpu.roll(x, 1, 0)) for x in rows[-HALF_Y:]]
        after = [jnp.where(sub == SUB - 1, 0.0, pltpu.roll(x, SUB - 1, 0)) for x in rows[:HALF_Y]]
        ext = before + rows + after
        two = [ext[2 * k] + ext[2 * k + 1] for k in range(GROUPS // 2 + 2)]
        four = [two[k] + two[k + 1] for k in range(GROUPS // 2 + 1)]
        out = []
        for k in range(GROUPS // 2):
            out.append(four[k] + ext[2 * k + 4])
            out.append(ext[2 * k + 1] + four[k + 1])
        return out

    def covariances(p, carry):
        for q in range(per_date):
            off = p * per_date + q
            source = flipped(me, turns, off)

            @pl.when(off != 0)
            def _():
                pltpu.make_async_remote_copy(
                    src_ref=block(source), dst_ref=win.at[source], send_sem=ssem.at[off],
                    recv_sem=rsem.at[off], device_id={"pix": source}, device_id_type=MESH,
                ).wait_recv()

        for q in range(per_date):
            source = date_at(p) * per_date + q
            for c in range(2):
                stage[p, c, q * local_rows:(q + 1) * local_rows] = win[source, c].astype(f32)
        for c in range(2):
            lines = [stage[p, c, pl.ds(g, SUB, stride=GROUPS), :] for g in range(GROUPS)]
            zb[p, c] = jnp.concatenate(lines, axis=0).astype(bf16)

        def chunk(n, carry):
            one = zb[p, 0], zb[p, 1]
            margins = pair_products(
                (wide[p, 0], wide[p, 1]), (edge[n * CHUNK // PACK, 0], edge[n * CHUNK // PACK, 1])
            )
            planes = []
            for q in range(CHUNK):
                k = n * CHUNK + q
                keep = tall(mask[lax.rem(k, PACK)])
                for value, margin in zip(pair_products(one, (zb[k, 0], zb[k, 1])), margins):
                    planes.append(jnp.concatenate([value, margin * keep], axis=1))
            summed[...] = jnp.dot(
                jnp.concatenate(planes, axis=0), both[...], preferred_element_type=f32
            )
            for q in range(CHUNK):
                sums = [
                    window_sums(summed[(2 * q + part) * ROWS:(2 * q + part + 1) * ROWS])
                    for part in range(2)
                ]
                for g in range(GROUPS):
                    real, imag = sums[0][g], sums[1][g]
                    cov[g, p, n * CHUNK + q, 0] = real
                    cov[g, p, n * CHUNK + q, 1] = real + imag
                    cov[g, p, n * CHUNK + q, 2] = imag - real
            return carry

        lax.fori_loop(0, p // CHUNK + 1, chunk, 0)
        for g in range(GROUPS):
            cov[g, p, p, 0] = cov[g, p, p, 0] + load[g]
        return carry

    lax.fori_loop(0, DATES, covariances, 0)

    ref = flipped(my_date, date_turns, ref_ref[0])

    def send(turn):
        for off in range(1, devices):
            pltpu.make_async_remote_copy(
                src_ref=tile.at[turn, off // per_date], dst_ref=o_ref.at[me, turn],
                send_sem=ts.at[off], recv_sem=tr.at[off],
                device_id={"pix": peers[off]}, device_id_type=MESH,
            ).start()
        pltpu.make_async_copy(tile.at[turn, 0], o_ref.at[me, turn], local.at[8]).start()

    def solve(g, carry):
        for i in range(DATES):
            one, two = jnp.maximum(ref, i), jnp.minimum(ref, i)
            real = cov[g, one, two, 0]
            imag = 0.5 * (cov[g, one, two, 1] + cov[g, one, two, 2])
            sign = jnp.where(ref == i, 0.0, jnp.where(ref < i, 1.0, -1.0))
            imag = imag * sign
            vec[0, i, 0] = real
            vec[0, i, 1] = imag
            vec[0, i, 2] = real + imag

        def step(t, carry):
            src = lax.rem(t, 2)
            for base in range(0, DATES, SPAN):
                acc = [[None] * 3 for _ in range(SPAN)]
                for j in range(DATES):
                    vr, vi, vs = vec[src, j, 0], vec[src, j, 1], vec[src, j, 2]
                    for q in range(SPAN):
                        i = base + q
                        one, two = max(i, j), min(i, j)
                        cr = cov[g, one, two, 0]
                        if i == j:
                            terms, minus = (None, cr * vr, cr * vi), (False, True, False)
                        elif i > j:
                            terms = (cr * vs, cov[g, i, j, 1] * vi, cov[g, i, j, 2] * vr)
                            minus = (False, False, False)
                        else:
                            terms = (cr * vs, cov[g, j, i, 2] * vi, cov[g, j, i, 1] * vr)
                            minus = (False, True, True)
                        for n in range(3):
                            if terms[n] is None:
                                continue
                            if acc[q][n] is None:
                                acc[q][n] = -terms[n] if minus[n] else terms[n]
                            elif minus[n]:
                                acc[q][n] = acc[q][n] - terms[n]
                            else:
                                acc[q][n] = acc[q][n] + terms[n]
                for q in range(SPAN):
                    real, imag = acc[q][0] - acc[q][1], acc[q][0] + acc[q][2]
                    vec[1 - src, base + q, 0] = real
                    vec[1 - src, base + q, 1] = imag
                    vec[1 - src, base + q, 2] = real + imag
            return carry

        lax.fori_loop(0, POWER_ITERS - 1, step, 0)
        last = (POWER_ITERS - 1) % 2
        total = jnp.zeros((SUB, columns), f32)
        for k in range(DATES):
            vr, vi = vec[last, k, 0], vec[last, k, 1]
            total = total + (vr * vr + vi * vi)
        scale = DATES / total
        rr, ri = vec[last, ref, 0] * scale, vec[last, ref, 1] * scale
        comp_r = jnp.zeros_like(total)
        comp_i = jnp.zeros_like(total)
        turn = g // TURN
        at = pl.ds(pl.multiple_of(lax.rem(g, TURN) * 2 * SUB, 2 * SUB), 2 * SUB)
        for k in range(DATES):
            vr, vi = vec[last, k, 0], vec[last, k, 1]
            lr = vr * rr + vi * ri
            li = vi * rr - vr * ri
            zr = stage[k, 0, pl.ds(g, SUB, stride=GROUPS), :]
            zi = stage[k, 1, pl.ds(g, SUB, stride=GROUPS), :]
            comp_r = comp_r + (lr * zr + li * zi)
            comp_i = comp_i + (lr * zi - li * zr)
            tile[turn, k, at] = jnp.concatenate([lr, li], axis=0).astype(bf16)
        comp_ref[0, g] = comp_r * (1.0 / math.sqrt(DATES))
        comp_ref[1, g] = comp_i * (1.0 / math.sqrt(DATES))

        @pl.when((lax.rem(g, TURN) == 0) & (g > 0))
        def _():
            send(turn - 1)

        return carry

    lax.fori_loop(0, GROUPS, solve, 0)
    for c in mains:
        c.wait_send()
    send(TURNS - 1)

    whole = tile.at[:, 0]
    for off in range(1, devices):
        pltpu.make_async_remote_copy(
            src_ref=whole, dst_ref=o_ref.at[me], send_sem=ts.at[off], recv_sem=tr.at[off],
            device_id={"pix": peers[off]}, device_id_type=MESH,
        ).wait()
    pltpu.make_async_copy(whole, o_ref.at[me], local.at[8]).wait()


def spectrum_kernel(got_ref, table_ref, comp_ref, o_ref, out_ref, got, out, ins, outs):
    devices, columns = got.shape[0], got.shape[3]
    local_rows = out.shape[1]
    parts = ins.shape[0]
    size = devices // parts

    def copy_in(n):
        at = pl.ds(n * size, size)
        return pltpu.make_async_copy(got_ref.at[at], got.at[at], ins.at[n])

    def copy_out(n):
        at = pl.ds(n * size * columns, size * columns)
        return pltpu.make_async_copy(out.at[:, :, at], o_ref.at[:, :, at], outs.at[n])

    for n in range(parts):
        copy_in(n).start()
    for c in range(2):
        for g in range(GROUPS):
            out_ref[c, pl.ds(g, SUB, stride=GROUPS), :] = comp_ref[c, g]
    for n in range(parts):
        copy_in(n).wait()
        for m in range(0, size, 2):
            at = n * size + m
            both = jnp.concatenate(
                [got[at].reshape(2 * ROWS, columns), got[at + 1].reshape(2 * ROWS, columns)], axis=1
            )
            value = jnp.dot(
                table_ref[...], jnp.concatenate([both, both], axis=0), preferred_element_type=jnp.float32
            )
            for c in range(2):
                out[c, :, at * columns:(at + 2) * columns] = value[c * local_rows:(c + 1) * local_rows]
        copy_out(n).start()
    for n in range(parts):
        copy_out(n).wait()


def on_device(slcs, ref_date):
    devices = lax.axis_size("pix")
    local_rows, strip_columns = slcs.shape[1], slcs.shape[2]
    columns = strip_columns // devices
    per_date = ROWS // local_rows

    anywhere = pl.BlockSpec(memory_space=pl.ANY)
    vmem = pl.BlockSpec(memory_space=pltpu.VMEM)
    both, pick, order = window_weights(columns), pick_weights(columns), order_weights(local_rows)
    spread, mask = spread_weights()
    table = dct_weights(local_rows)
    f32, bf16 = jnp.float32, jnp.bfloat16
    sems = pltpu.SemaphoreType.DMA((devices,))
    phases, compressed = pl.pallas_call(
        functools.partial(link_kernel, devices),
        out_shape=(
            jax.ShapeDtypeStruct((devices, TURNS, TURN * 2 * SUB, columns), bf16),
            jax.ShapeDtypeStruct((2, GROUPS, SUB, columns), f32),
        ),
        in_specs=[pl.BlockSpec(memory_space=pltpu.SMEM)] + [anywhere] * 6,
        out_specs=(anywhere, vmem),
        scratch_shapes=[
            pltpu.VMEM((2, local_rows, strip_columns + 2 * columns), bf16),
            pltpu.VMEM((devices, 2, local_rows, columns), bf16),
            pltpu.VMEM((devices, HALO, LANES), bf16),
            pltpu.VMEM((devices, HALO, LANES), bf16),
            pltpu.VMEM((DATES * HALO, per_date * LANES), bf16),
            pltpu.VMEM((DATES // PACK, 2, ROWS, LANES), bf16),
            pltpu.VMEM((DATES, 2, ROWS, LANES), bf16),
            pltpu.VMEM(both.shape, bf16),
            pltpu.VMEM(pick.shape, bf16),
            pltpu.VMEM(order.shape, bf16),
            pltpu.VMEM(spread.shape, bf16),
            pltpu.VMEM(mask.shape, bf16),
            pltpu.VMEM((DATES, 2, ROWS, columns), f32),
            pltpu.VMEM((DATES, 2, ROWS, columns), bf16),
            pltpu.VMEM((2 * CHUNK * ROWS, columns), f32),
            pltpu.VMEM((GROUPS, SUB, columns), f32),
            pltpu.VMEM((GROUPS, DATES, DATES, 3, SUB, columns), f32),
            pltpu.VMEM((2, DATES, 3, SUB, columns), f32),
            pltpu.VMEM((TURNS, DATES, TURN * 2 * SUB, columns), bf16),
            pltpu.SemaphoreType.DMA((9,)),
        ] + [sems] * 6,
        compiler_params=pltpu.CompilerParams(
            collective_id=0, has_side_effects=True, vmem_limit_bytes=60 * 1024 * 1024
        ),
        name="link",
    )(ref_date, slcs, both, pick, order, spread, mask)

    if per_date > 1:
        table = lax.dynamic_index_in_dim(table, lax.rem(lax.axis_index("pix"), per_date), 0, False)
    else:
        table = table[0]
    parts = 4
    return pl.pallas_call(
        spectrum_kernel,
        out_shape=(
            jax.ShapeDtypeStruct((2, local_rows, strip_columns), f32),
            jax.ShapeDtypeStruct((2, ROWS, columns), f32),
        ),
        in_specs=[anywhere, vmem, vmem],
        out_specs=(anywhere, vmem),
        scratch_shapes=[
            pltpu.VMEM((devices, TURNS, TURN * 2 * SUB, columns), bf16),
            pltpu.VMEM((2, local_rows, strip_columns), f32),
            pltpu.SemaphoreType.DMA((parts,)),
            pltpu.SemaphoreType.DMA((parts,)),
        ],
        name="spectrum",
    )(phases, table, compressed)


def solution(mesh):
    return jax.shard_map(
        on_device,
        mesh=mesh,
        in_specs=(P(None, ("grp", "pix"), None), P("grp")),
        out_specs=(P(None, ("grp", "pix"), None), P(None, None, ("grp", "pix"))),
        check_vma=False,
    )
```

```python
import functools
import math

import jax
import jax.numpy as jnp
import numpy as np
from jax import lax
from jax.experimental import pallas as pl
from jax.experimental.pallas import tpu as pltpu
from jax.sharding import PartitionSpec as P

DATES = 16
ROWS = 64
HALF_X = 5
HALF_Y = 2
POWER_ITERS = 6
LOADING = 0.25

LANES = 128
SUB = 8
GROUPS = ROWS // SUB
HALO = 16
PACK = LANES // HALO
CHUNK = 4
SPAN = 8
SCALE = 2.0 ** -6
MESH = pl.DeviceIdType.MESH


def window_weights(columns):
    target = np.arange(columns)[None, :]
    band = np.abs(np.arange(columns)[:, None] - target) <= HALF_X
    outside = np.concatenate([np.arange(-HALF_X, 0), columns + np.arange(HALF_X)])
    halo = np.zeros((HALO, columns), np.float32)
    halo[: 2 * HALF_X] = np.abs(outside[:, None] - target) <= HALF_X
    both = np.concatenate([band.astype(np.float32), np.tile(halo, (PACK, 1))], axis=0)
    return jnp.asarray(both * SCALE, jnp.bfloat16)


def pick_weights(columns):
    pick = np.zeros((HALO, 2 * columns), np.float32)
    for h in range(HALF_X):
        pick[h, columns - HALF_X + h] = 1.0
        pick[HALF_X + h, columns + h] = 1.0
    return jnp.asarray(pick, jnp.bfloat16)


def order_weights(local_rows):
    per_date = ROWS // local_rows
    order = np.zeros((2, GROUPS, SUB, per_date, LANES), np.float32)
    for c in range(2):
        for line in range(ROWS):
            q, r = divmod(line, local_rows)
            order[c, line % GROUPS, line // GROUPS, q, c * local_rows + r] = 1.0
    return jnp.asarray(order.reshape(2 * ROWS, per_date * LANES), jnp.bfloat16)


def block_masks():
    block = np.arange(PACK)[:, None, None] == (np.arange(LANES) // HALO)[None, None, :]
    return jnp.asarray(np.broadcast_to(block, (PACK, 2 * SUB, LANES)), jnp.float32)


def dct_weights(local_rows):
    frequency = np.arange(ROWS, dtype=np.float64)[:, None]
    position = np.arange(ROWS, dtype=np.float64)[None, :]
    weight = np.where(frequency == 0, math.sqrt(1.0 / ROWS), math.sqrt(2.0 / ROWS))
    table = weight * np.cos(np.pi * (2.0 * position + 1.0) * frequency / (2.0 * ROWS))
    table = table.reshape(ROWS // local_rows, local_rows, SUB, GROUPS).transpose(0, 1, 3, 2)
    big = np.zeros((ROWS // local_rows, 2, local_rows, GROUPS, 2, SUB), np.float32)
    for c in range(2):
        big[:, c, :, :, c] = table
    big = big.reshape(ROWS // local_rows, 2 * local_rows, 2 * ROWS)
    high = big.astype(jnp.bfloat16)
    low = (big - high.astype(np.float32)).astype(jnp.bfloat16)
    return jnp.asarray(np.concatenate([high, low], axis=2))


def pair_products(one, two):
    real = one[0] * two[0] + one[1] * two[1]
    imag = one[1] * two[0] - one[0] * two[1]
    return real, imag


def tall_of(value, rows):
    return jnp.concatenate([value] * (rows // value.shape[0]), axis=0)


def flips(a, size):
    out, bit = [], 1
    while bit < size:
        out.append(bit - 2 * bit * ((a // bit) % 2))
        bit *= 2
    return out


def flipped(a, deltas, b):
    for n, delta in enumerate(deltas):
        if isinstance(b, int):
            a = a + delta if (b >> n) & 1 else a
        else:
            a = a + delta * ((b // (1 << n)) % 2)
    return a


def link_kernel(devices, ref_ref, x_ref, both_ref, pick_ref, order_ref, mask_ref,
                o_ref, comp_ref,
                xs, win, hsend, hwin, edge, wide, both, pick, order, mask,
                stage, zb, summed, load, cov, vec, tile, comp,
                local, ssem, rsem, hs, hr, ts, tr):
    columns = win.shape[3]
    local_rows = win.shape[2]
    strip_columns = x_ref.shape[2]
    per_date = ROWS // local_rows
    me = lax.axis_index("pix")
    my_date = me // per_date
    turns = flips(me, devices)
    date_turns = turns[(per_date - 1).bit_length():]
    peers = [flipped(me, turns, off) for off in range(devices)]
    bf16, f32 = jnp.bfloat16, jnp.float32

    barrier = pltpu.get_barrier_semaphore()
    for peer in peers[1:]:
        pl.semaphore_signal(barrier, inc=1, device_id={"pix": peer}, device_id_type=MESH)

    def block(n):
        return x_ref.at[:, :, pl.ds(pl.multiple_of(n * columns, columns), columns)]

    loads = [
        pltpu.make_async_copy(src, dst, local.at[n])
        for n, (src, dst) in enumerate((
            (x_ref, xs.at[:, :, columns:columns + strip_columns]),
            (pick_ref, pick), (block(me), win.at[me]), (both_ref, both), (order_ref, order),
            (mask_ref, mask),
        ))
    ]
    for copy in loads:
        copy.start()

    def main_copy(off, peer):
        return pltpu.make_async_remote_copy(
            src_ref=block(peer), dst_ref=win.at[me], send_sem=ssem.at[off], recv_sem=rsem.at[off],
            device_id={"pix": peer}, device_id_type=MESH,
        )

    def halo_copy(off, peer):
        return pltpu.make_async_remote_copy(
            src_ref=hsend.at[peer], dst_ref=hwin.at[me], send_sem=hs.at[off],
            recv_sem=hr.at[off], device_id={"pix": peer}, device_id_type=MESH,
        )

    first = sorted({1, 2, 3, devices // 4, 3 * devices // 4, 3 * devices // 4 + 1})
    later = [off for off in range(1, devices) if off not in first]
    halos = [halo_copy(off, peers[off]) for off in range(1, devices)]
    mains = {off: main_copy(off, peers[off]) for off in range(1, devices)}

    pl.semaphore_wait(barrier, devices - 1)
    for off in first:
        mains[off].start()

    margin = jnp.zeros((2, local_rows, columns), bf16)
    xs[:, :, 0:columns] = margin
    xs[:, :, columns + strip_columns:2 * columns + strip_columns] = margin
    loads[0].wait()
    loads[1].wait()

    blocks = min(devices, 16)

    def cut_halos(n, carry):
        for q in range(blocks):
            at = (n * blocks + q) * columns
            left = xs[:, :, pl.ds(pl.multiple_of(at, columns), columns)]
            right = xs[:, :, pl.ds(pl.multiple_of(at + 2 * columns, columns), columns)]
            near = jnp.concatenate(
                [left.reshape(2 * local_rows, columns), right.reshape(2 * local_rows, columns)], axis=1
            )
            if 2 * local_rows < LANES:
                fill = jnp.zeros((LANES - 2 * local_rows, 2 * columns), bf16)
                near = jnp.concatenate([near, fill], axis=0)
            got = lax.dot_general(
                pick[...], near, (((1,), (1,)), ((), ())), preferred_element_type=f32
            )
            hsend[n * blocks + q] = got.astype(bf16)
        return carry

    lax.fori_loop(0, devices // blocks, cut_halos, 0)
    hwin[me] = hsend[me]
    for c in halos:
        c.start()
    for off in later:
        mains[off].start()

    first_column = me * columns
    sub = lax.broadcasted_iota(jnp.int32, (SUB, columns), 0)
    lane = lax.broadcasted_iota(jnp.int32, (SUB, columns), 1) + first_column
    across = jnp.minimum(lane + HALF_X, strip_columns - 1) - jnp.maximum(lane - HALF_X, 0) + 1
    for g in range(GROUPS):
        line = sub * GROUPS + g
        along = jnp.minimum(line + HALF_Y, ROWS - 1) - jnp.maximum(line - HALF_Y, 0) + 1
        load[g] = (along * across).astype(f32) * (LOADING * SCALE)
    edge[...] = jnp.zeros_like(edge)
    for copy in loads[2:]:
        copy.wait()

    def date_at(p):
        return flipped(my_date, date_turns, p)

    def tall(value):
        return tall_of(value, ROWS)

    def window_sums(plane):
        rows = [plane[g * SUB:(g + 1) * SUB] for g in range(GROUPS)]
        before = [jnp.where(sub == 0, 0.0, pltpu.roll(x, 1, 0)) for x in rows[-HALF_Y:]]
        after = [jnp.where(sub == SUB - 1, 0.0, pltpu.roll(x, SUB - 1, 0)) for x in rows[:HALF_Y]]
        ext = before + rows + after
        two = [ext[2 * k] + ext[2 * k + 1] for k in range(GROUPS // 2 + 2)]
        four = [two[k] + two[k + 1] for k in range(GROUPS // 2 + 1)]
        out = []
        for k in range(GROUPS // 2):
            out.append(four[k] + ext[2 * k + 4])
            out.append(ext[2 * k + 1] + four[k + 1])
        return out

    def finish(p, n):
        for q in range(CHUNK):
            sums = [
                window_sums(summed[(2 * q + part) * ROWS:(2 * q + part + 1) * ROWS])
                for part in range(2)
            ]
            for g in range(GROUPS):
                real, imag = sums[0][g], sums[1][g]
                cov[g, p, n * CHUNK + q, 0] = real
                cov[g, p, n * CHUNK + q, 1] = real + imag
                cov[g, p, n * CHUNK + q, 2] = imag - real

    def begin(p, n):
        one = zb[p, 0].astype(bf16), zb[p, 1].astype(bf16)
        half = (n * CHUNK) // PACK
        margins = pair_products(
            (wide[0].astype(bf16), wide[1].astype(bf16)),
            (edge[half, 0].astype(bf16), edge[half, 1].astype(bf16)),
        )
        planes = []
        for q in range(CHUNK):
            k = n * CHUNK + q
            two = zb[k, 0].astype(bf16), zb[k, 1].astype(bf16)
            keep = tall(mask[k - half * PACK].astype(bf16))
            for value, margin in zip(pair_products(one, two), margins):
                planes.append(jnp.concatenate([value, margin * keep], axis=1))
        summed[...] = jnp.dot(
            jnp.concatenate(planes, axis=0), both[...], preferred_element_type=f32
        )

    def covariances(p, prev):
        sources = []
        for q in range(per_date):
            off = p * per_date + q
            source = flipped(me, turns, off)
            sources.append(source)

            @pl.when(off != 0)
            def _():
                pltpu.make_async_remote_copy(
                    src_ref=hsend.at[source], dst_ref=hwin.at[source], send_sem=hs.at[off],
                    recv_sem=hr.at[off], device_id={"pix": source}, device_id_type=MESH,
                ).wait_recv()
                pltpu.make_async_remote_copy(
                    src_ref=block(source), dst_ref=win.at[source], send_sem=ssem.at[off],
                    recv_sem=rsem.at[off], device_id={"pix": source}, device_id_type=MESH,
                ).wait_recv()

        sources = [date_at(p) * per_date + q for q in range(per_date)]
        margin = jnp.concatenate([tall_of(hwin[source], LANES) for source in sources], axis=1)
        got = lax.dot_general(
            order[...], margin, (((1,), (1,)), ((), ())), preferred_element_type=f32
        )
        keep = tall(mask[lax.rem(p, PACK)])
        half = p // PACK
        for c in range(2):
            part = got[c * ROWS:(c + 1) * ROWS]
            wide[c] = part
            edge[half, c] = edge[half, c] + part * keep
        for q, source in enumerate(sources):
            for c in range(2):
                stage[c, q * local_rows:(q + 1) * local_rows] = win[source, c].astype(f32)
        for c in range(2):
            for g in range(GROUPS):
                zb[p, c, g * SUB:(g + 1) * SUB] = stage[c, pl.ds(g, SUB, stride=GROUPS), :]

        def chunk(n, prev):
            finish(*prev)
            begin(p, n)
            return p, n

        return lax.fori_loop(0, p // CHUNK + 1, chunk, prev)

    finish(*lax.fori_loop(0, DATES, covariances, (jnp.int32(0), jnp.int32(0))))

    ref = flipped(my_date, date_turns, ref_ref[0])

    def send(g):
        for off in range(1, devices):
            pltpu.make_async_remote_copy(
                src_ref=tile.at[g, off // per_date], dst_ref=o_ref.at[me, g],
                send_sem=ts.at[off], recv_sem=tr.at[off],
                device_id={"pix": peers[off]}, device_id_type=MESH,
            ).start()
        pltpu.make_async_copy(tile.at[g, 0], o_ref.at[me, g], local.at[6]).start()

    def solve(g, carry):
        for i in range(DATES):
            cov[g, i, i, 0] = cov[g, i, i, 0] + load[g]
        for i in range(DATES):
            one, two = jnp.maximum(ref, i), jnp.minimum(ref, i)
            real = cov[g, one, two, 0]
            imag = 0.5 * (cov[g, one, two, 1] + cov[g, one, two, 2])
            sign = jnp.where(ref == i, 0.0, jnp.where(ref < i, 1.0, -1.0))
            imag = imag * sign
            vec[0, i, 0] = real
            vec[0, i, 1] = imag
            vec[0, i, 2] = real + imag

        @pl.when(g > 0)
        def _():
            send(g - 1)

        def step(t, carry):
            src = lax.rem(t, 2)
            for base in range(0, DATES, SPAN):
                acc = [[None] * 3 for _ in range(SPAN)]
                for j in range(DATES):
                    vr, vi, vs = vec[src, j, 0], vec[src, j, 1], vec[src, j, 2]
                    for q in range(SPAN):
                        i = base + q
                        one, two = max(i, j), min(i, j)
                        cr = cov[g, one, two, 0]
                        if i == j:
                            terms, minus = (None, cr * vr, cr * vi), (False, True, False)
                        elif i > j:
                            terms = (cr * vs, cov[g, i, j, 1] * vi, cov[g, i, j, 2] * vr)
                            minus = (False, False, False)
                        else:
                            terms = (cr * vs, cov[g, j, i, 2] * vi, cov[g, j, i, 1] * vr)
                            minus = (False, True, True)
                        for n in range(3):
                            if terms[n] is None:
                                continue
                            if acc[q][n] is None:
                                acc[q][n] = -terms[n] if minus[n] else terms[n]
                            elif minus[n]:
                                acc[q][n] = acc[q][n] - terms[n]
                            else:
                                acc[q][n] = acc[q][n] + terms[n]
                for q in range(SPAN):
                    real, imag = acc[q][0] - acc[q][1], acc[q][0] + acc[q][2]
                    vec[1 - src, base + q, 0] = real
                    vec[1 - src, base + q, 1] = imag
                    vec[1 - src, base + q, 2] = real + imag
            return carry

        lax.fori_loop(0, POWER_ITERS - 1, step, 0)
        last = (POWER_ITERS - 1) % 2
        total = jnp.zeros((SUB, columns), f32)
        for k in range(DATES):
            vr, vi = vec[last, k, 0], vec[last, k, 1]
            total = total + (vr * vr + vi * vi)
        scale = DATES / total
        rr, ri = vec[last, ref, 0] * scale, vec[last, ref, 1] * scale
        comp_r = jnp.zeros_like(total)
        comp_i = jnp.zeros_like(total)
        at = pl.ds(pl.multiple_of(g * SUB, SUB), SUB)
        for k in range(DATES):
            vr, vi = vec[last, k, 0], vec[last, k, 1]
            lr = vr * rr + vi * ri
            li = vi * rr - vr * ri
            zr, zi = zb[k, 0, at], zb[k, 1, at]
            comp_r = comp_r + (lr * zr + li * zi)
            comp_i = comp_i + (lr * zi - li * zr)
            tile[g, k] = jnp.concatenate([lr, li], axis=0).astype(bf16)
        comp[0, g] = comp_r * (1.0 / math.sqrt(DATES))
        comp[1, g] = comp_i * (1.0 / math.sqrt(DATES))
        return carry

    lax.fori_loop(0, GROUPS, solve, 0)
    for c in halos:
        c.wait_send()
    send(GROUPS - 1)
    out = pltpu.make_async_copy(comp, comp_ref, local.at[7])
    out.start()
    for off in range(1, devices):
        mains[off].wait_send()

    whole = tile.at[:, 0]
    for off in range(1, devices):
        pltpu.make_async_remote_copy(
            src_ref=whole, dst_ref=o_ref.at[me], send_sem=ts.at[off], recv_sem=tr.at[off],
            device_id={"pix": peers[off]}, device_id_type=MESH,
        ).wait()
    pltpu.make_async_copy(whole, o_ref.at[me], local.at[6]).wait()
    out.wait()


def spectrum_kernel(got_ref, table_ref, comp_ref, o_ref, out_ref, got, table, comp, order, out, ins, outs):
    devices, columns = got.shape[0], got.shape[3]
    local_rows = out.shape[1]
    parts = outs.shape[0] - 1
    size = devices // parts

    def copy_in(n):
        at = pl.ds(n * size, size)
        return pltpu.make_async_copy(got_ref.at[at], got.at[at], ins.at[n])

    def copy_out(n):
        at = pl.ds(n * size * columns, size * columns)
        return pltpu.make_async_copy(out.at[:, :, at], o_ref.at[:, :, at], outs.at[n])

    tables = pltpu.make_async_copy(table_ref, table, ins.at[parts])
    comps = pltpu.make_async_copy(comp_ref, comp, ins.at[parts + 1])
    tables.start()
    for n in range(parts):
        copy_in(n).start()
    comps.start()
    tables.wait()
    for n in range(parts):
        copy_in(n).wait()
        for m in range(0, size, 2):
            at = n * size + m
            both = jnp.concatenate(
                [got[at].reshape(2 * ROWS, columns), got[at + 1].reshape(2 * ROWS, columns)], axis=1
            )
            value = jnp.dot(
                table[...], jnp.concatenate([both, both], axis=0), preferred_element_type=jnp.float32
            )
            for c in range(2):
                out[c, :, at * columns:(at + 2) * columns] = value[c * local_rows:(c + 1) * local_rows]
        copy_out(n).start()
    comps.wait()
    for c in range(2):
        for g in range(GROUPS):
            order[c, pl.ds(g, SUB, stride=GROUPS), :] = comp[c, g]
    last = pltpu.make_async_copy(order, out_ref, outs.at[parts])
    last.start()
    for n in range(parts):
        copy_out(n).wait()
    last.wait()


def on_device(slcs, ref_date):
    devices = lax.axis_size("pix")
    local_rows, strip_columns = slcs.shape[1], slcs.shape[2]
    columns = strip_columns // devices
    per_date = ROWS // local_rows

    anywhere = pl.BlockSpec(memory_space=pl.ANY)
    both, pick, order = window_weights(columns), pick_weights(columns), order_weights(local_rows)
    mask = block_masks()
    table = dct_weights(local_rows)
    f32, bf16 = jnp.float32, jnp.bfloat16
    sems = pltpu.SemaphoreType.DMA((devices,))
    phases, compressed = pl.pallas_call(
        functools.partial(link_kernel, devices),
        out_shape=(
            jax.ShapeDtypeStruct((devices, GROUPS, 2 * SUB, columns), bf16),
            jax.ShapeDtypeStruct((2, GROUPS, SUB, columns), f32),
        ),
        in_specs=[pl.BlockSpec(memory_space=pltpu.SMEM)] + [anywhere] * 5,
        out_specs=(anywhere, anywhere),
        scratch_shapes=[
            pltpu.VMEM((2, local_rows, strip_columns + 2 * columns), bf16),
            pltpu.VMEM((devices, 2, local_rows, columns), bf16),
            pltpu.VMEM((devices, HALO, LANES), bf16),
            pltpu.VMEM((devices, HALO, LANES), bf16),
            pltpu.VMEM((DATES // PACK, 2, ROWS, LANES), f32),
            pltpu.VMEM((2, ROWS, LANES), f32),
            pltpu.VMEM(both.shape, bf16),
            pltpu.VMEM(pick.shape, bf16),
            pltpu.VMEM(order.shape, bf16),
            pltpu.VMEM(mask.shape, f32),
            pltpu.VMEM((2, ROWS, columns), f32),
            pltpu.VMEM((DATES, 2, ROWS, columns), f32),
            pltpu.VMEM((2 * CHUNK * ROWS, columns), f32),
            pltpu.VMEM((GROUPS, SUB, columns), f32),
            pltpu.VMEM((GROUPS, DATES, DATES, 3, SUB, columns), f32),
            pltpu.VMEM((2, DATES, 3, SUB, columns), f32),
            pltpu.VMEM((GROUPS, DATES, 2 * SUB, columns), bf16),
            pltpu.VMEM((2, GROUPS, SUB, columns), f32),
            pltpu.SemaphoreType.DMA((8,)),
        ] + [sems] * 6,
        compiler_params=pltpu.CompilerParams(
            collective_id=0, has_side_effects=True, vmem_limit_bytes=60 * 1024 * 1024
        ),
        name="link",
    )(ref_date, slcs, both, pick, order, mask)

    if per_date > 1:
        table = lax.dynamic_index_in_dim(table, lax.rem(lax.axis_index("pix"), per_date), 0, False)
    else:
        table = table[0]
    parts = 4
    return pl.pallas_call(
        spectrum_kernel,
        out_shape=(
            jax.ShapeDtypeStruct((2, local_rows, strip_columns), f32),
            jax.ShapeDtypeStruct((2, ROWS, columns), f32),
        ),
        in_specs=[anywhere] * 3,
        out_specs=(anywhere, anywhere),
        scratch_shapes=[
            pltpu.VMEM((devices, GROUPS, 2 * SUB, columns), bf16),
            pltpu.VMEM(table.shape, bf16),
            pltpu.VMEM((2, GROUPS, SUB, columns), f32),
            pltpu.VMEM((2, ROWS, columns), f32),
            pltpu.VMEM((2, local_rows, strip_columns), f32),
            pltpu.SemaphoreType.DMA((parts + 2,)),
            pltpu.SemaphoreType.DMA((parts + 1,)),
        ],
        name="spectrum",
    )(phases, table, compressed)


def solution(mesh):
    return jax.shard_map(
        on_device,
        mesh=mesh,
        in_specs=(P(None, ("grp", "pix"), None), P("grp")),
        out_specs=(P(None, ("grp", "pix"), None), P(None, None, ("grp", "pix"))),
        check_vma=False,
    )
```

```python
import functools
import math

import jax
import jax.numpy as jnp
import numpy as np
from jax import lax
from jax.experimental import pallas as pl
from jax.experimental.pallas import tpu as pltpu
from jax.sharding import PartitionSpec as P

DATES = 16
ROWS = 64
HALF_X = 5
HALF_Y = 2
POWER_ITERS = 6
LOADING = 0.25

LANES = 128
SUB = 8
GROUPS = ROWS // SUB
HALO = 16
PACK = LANES // HALO
CHUNK = 8
SPAN = 8
SCALE = 2.0 ** -6
MESH = pl.DeviceIdType.MESH


def window_weights(columns):
    target = np.arange(columns)[None, :]
    band = np.abs(np.arange(columns)[:, None] - target) <= HALF_X
    outside = np.concatenate([np.arange(-HALF_X, 0), columns + np.arange(HALF_X)])
    halo = np.zeros((HALO, columns), np.float32)
    halo[: 2 * HALF_X] = np.abs(outside[:, None] - target) <= HALF_X
    both = np.concatenate([band.astype(np.float32), np.tile(halo, (PACK, 1))], axis=0)
    return jnp.asarray(both * SCALE, jnp.bfloat16)


def pick_weights(columns):
    pick = np.zeros((HALO, 2 * columns), np.float32)
    for h in range(HALF_X):
        pick[h, columns - HALF_X + h] = 1.0
        pick[HALF_X + h, columns + h] = 1.0
    return jnp.asarray(pick, jnp.bfloat16)


def order_weights(local_rows):
    per_date = ROWS // local_rows
    order = np.zeros((2, GROUPS, SUB, per_date, LANES), np.float32)
    for c in range(2):
        for line in range(ROWS):
            q, r = divmod(line, local_rows)
            order[c, line % GROUPS, line // GROUPS, q, c * local_rows + r] = 1.0
    return jnp.asarray(order.reshape(2 * ROWS, per_date * LANES), jnp.bfloat16)


def block_masks():
    block = np.arange(PACK)[:, None, None] == (np.arange(LANES) // HALO)[None, None, :]
    return jnp.asarray(np.broadcast_to(block, (PACK, 2 * SUB, LANES)), jnp.float32)


def dct_weights(local_rows):
    frequency = np.arange(ROWS, dtype=np.float64)[:, None]
    position = np.arange(ROWS, dtype=np.float64)[None, :]
    weight = np.where(frequency == 0, math.sqrt(1.0 / ROWS), math.sqrt(2.0 / ROWS))
    table = weight * np.cos(np.pi * (2.0 * position + 1.0) * frequency / (2.0 * ROWS))
    table = table.reshape(ROWS // local_rows, local_rows, SUB, GROUPS).transpose(0, 1, 3, 2)
    big = np.zeros((ROWS // local_rows, 2, local_rows, GROUPS, 2, SUB), np.float32)
    for c in range(2):
        big[:, c, :, :, c] = table
    big = big.reshape(ROWS // local_rows, 2 * local_rows, 2 * ROWS)
    high = big.astype(jnp.bfloat16)
    low = (big - high.astype(np.float32)).astype(jnp.bfloat16)
    return jnp.asarray(np.concatenate([high, low], axis=2))


def pair_products(one, two):
    real = one[0] * two[0] + one[1] * two[1]
    imag = one[1] * two[0] - one[0] * two[1]
    return real, imag


def tall_of(value, rows):
    return jnp.concatenate([value] * (rows // value.shape[0]), axis=0)


def flips(a, size):
    out, bit = [], 1
    while bit < size:
        out.append(bit - 2 * bit * ((a // bit) % 2))
        bit *= 2
    return out


def flipped(a, deltas, b):
    for n, delta in enumerate(deltas):
        if isinstance(b, int):
            a = a + delta if (b >> n) & 1 else a
        else:
            a = a + delta * ((b // (1 << n)) % 2)
    return a


def link_kernel(devices, ref_ref, x_ref, both_ref, pick_ref, order_ref, mask_ref,
                o_ref, comp_ref,
                xs, win, hsend, edge, wide, both, pick, order, mask,
                stage, zb, summed, load, cov, vec, tile, comp,
                local, sent, rsem, got_sem):
    columns = win.shape[2]
    height = x_ref.shape[0]
    local_rows = height // 2
    strip_columns = x_ref.shape[1]
    per_date = ROWS // local_rows
    me = lax.axis_index("pix")
    my_date = me // per_date
    turns = flips(me, devices)
    date_turns = turns[(per_date - 1).bit_length():]
    peers = [flipped(me, turns, off) for off in range(devices)]
    bf16, f32 = jnp.bfloat16, jnp.float32

    barrier = pltpu.get_barrier_semaphore()
    for peer in peers[1:]:
        pl.semaphore_signal(barrier, inc=1, device_id={"pix": peer}, device_id_type=MESH)

    def block(n):
        return x_ref.at[:, pl.ds(pl.multiple_of(n * columns, columns), columns)]

    loads = [
        pltpu.make_async_copy(src, dst, local.at[n])
        for n, (src, dst) in enumerate((
            (x_ref, xs.at[:, columns:columns + strip_columns]),
            (pick_ref, pick), (block(me), win.at[me, 0:height]), (both_ref, both), (order_ref, order),
            (mask_ref, mask),
        ))
    ]
    for copy in loads:
        copy.start()

    def main_copy(off, peer):
        return pltpu.make_async_remote_copy(
            src_ref=block(peer), dst_ref=win.at[me, 0:height], send_sem=sent.at[0],
            recv_sem=rsem.at[off], device_id={"pix": peer}, device_id_type=MESH,
        )

    def halo_copy(off, peer):
        return pltpu.make_async_remote_copy(
            src_ref=hsend.at[peer], dst_ref=win.at[me, height:height + HALO], send_sem=sent.at[0],
            recv_sem=rsem.at[off], device_id={"pix": peer}, device_id_type=MESH,
        )

    first = sorted({1, 2, 3, devices // 4, 3 * devices // 4, 3 * devices // 4 + 1})
    later = [off for off in range(1, devices) if off not in first]
    halos = [halo_copy(off, peers[off]) for off in range(1, devices)]
    mains = {off: main_copy(off, peers[off]) for off in range(1, devices)}

    pl.semaphore_wait(barrier, devices - 1)
    for off in first:
        mains[off].start()

    margin = jnp.zeros((height, columns), bf16)
    xs[:, 0:columns] = margin
    xs[:, columns + strip_columns:2 * columns + strip_columns] = margin
    loads[0].wait()
    loads[1].wait()

    blocks = min(devices, 16)

    def cut_halos(n, carry):
        for q in range(blocks):
            at = (n * blocks + q) * columns
            left = xs[:, pl.ds(pl.multiple_of(at, columns), columns)]
            right = xs[:, pl.ds(pl.multiple_of(at + 2 * columns, columns), columns)]
            near = jnp.concatenate([left, right], axis=1)
            if height < LANES:
                fill = jnp.zeros((LANES - height, 2 * columns), bf16)
                near = jnp.concatenate([near, fill], axis=0)
            got = lax.dot_general(
                pick[...], near, (((1,), (1,)), ((), ())), preferred_element_type=f32
            )
            hsend[n * blocks + q] = got.astype(bf16)
        return carry

    lax.fori_loop(0, devices // blocks, cut_halos, 0)
    win[me, height:height + HALO] = hsend[me]
    for c in halos:
        c.start()
    for off in later:
        mains[off].start()

    first_column = me * columns
    sub = lax.broadcasted_iota(jnp.int32, (SUB, columns), 0)
    lane = lax.broadcasted_iota(jnp.int32, (SUB, columns), 1) + first_column
    across = jnp.minimum(lane + HALF_X, strip_columns - 1) - jnp.maximum(lane - HALF_X, 0) + 1
    for g in range(GROUPS):
        line = sub * GROUPS + g
        along = jnp.minimum(line + HALF_Y, ROWS - 1) - jnp.maximum(line - HALF_Y, 0) + 1
        load[g] = (along * across).astype(f32) * (LOADING * SCALE)
    edge[...] = jnp.zeros_like(edge)
    for copy in loads[2:]:
        copy.wait()

    def date_at(p):
        return flipped(my_date, date_turns, p)

    def tall(value):
        return tall_of(value, ROWS)

    def window_sums(plane):
        rows = [plane[g * SUB:(g + 1) * SUB] for g in range(GROUPS)]
        before = [jnp.where(sub == 0, 0.0, pltpu.roll(x, 1, 0)) for x in rows[-HALF_Y:]]
        after = [jnp.where(sub == SUB - 1, 0.0, pltpu.roll(x, SUB - 1, 0)) for x in rows[:HALF_Y]]
        ext = before + rows + after
        two = [ext[2 * k] + ext[2 * k + 1] for k in range(GROUPS // 2 + 2)]
        four = [two[k] + two[k + 1] for k in range(GROUPS // 2 + 1)]
        out = []
        for k in range(GROUPS // 2):
            out.append(four[k] + ext[2 * k + 4])
            out.append(ext[2 * k + 1] + four[k + 1])
        return out

    def finish(p, n):
        for q in range(CHUNK):
            sums = [
                window_sums(summed[(2 * q + part) * ROWS:(2 * q + part + 1) * ROWS])
                for part in range(2)
            ]
            for g in range(GROUPS):
                real, imag = sums[0][g], sums[1][g]
                cov[g, p, n * CHUNK + q, 0] = real
                cov[g, p, n * CHUNK + q, 1] = real + imag
                cov[g, p, n * CHUNK + q, 2] = imag - real

    def begin(p, n):
        one = zb[p, 0].astype(bf16), zb[p, 1].astype(bf16)
        half = (n * CHUNK) // PACK
        margins = pair_products(
            (wide[0].astype(bf16), wide[1].astype(bf16)),
            (edge[half, 0].astype(bf16), edge[half, 1].astype(bf16)),
        )
        planes = []
        for q in range(CHUNK):
            k = n * CHUNK + q
            two = zb[k, 0].astype(bf16), zb[k, 1].astype(bf16)
            keep = tall(mask[k - half * PACK].astype(bf16))
            for value, margin in zip(pair_products(one, two), margins):
                planes.append(jnp.concatenate([value, margin * keep], axis=1))
        summed[...] = jnp.dot(
            jnp.concatenate(planes, axis=0), both[...], preferred_element_type=f32
        )

    def covariances(p, prev):
        for q in range(per_date):
            off = p * per_date + q
            source = flipped(me, turns, off)

            @pl.when(off != 0)
            def _():
                pltpu.make_async_remote_copy(
                    src_ref=win.at[source], dst_ref=win.at[source], send_sem=sent.at[0],
                    recv_sem=rsem.at[off], device_id={"pix": source}, device_id_type=MESH,
                ).wait_recv()

        sources = [date_at(p) * per_date + q for q in range(per_date)]
        margin = jnp.concatenate([tall_of(win[source, height:height + HALO], LANES) for source in sources], axis=1)
        got = lax.dot_general(
            order[...], margin, (((1,), (1,)), ((), ())), preferred_element_type=f32
        )
        keep = tall(mask[lax.rem(p, PACK)])
        half = p // PACK
        for c in range(2):
            part = got[c * ROWS:(c + 1) * ROWS]
            wide[c] = part
            edge[half, c] = edge[half, c] + part * keep
        for q, source in enumerate(sources):
            for c in range(2):
                stage[c, q * local_rows:(q + 1) * local_rows] = win[
                    source, c * local_rows:(c + 1) * local_rows
                ].astype(f32)
        for c in range(2):
            for g in range(GROUPS):
                zb[p, c, g * SUB:(g + 1) * SUB] = stage[c, pl.ds(g, SUB, stride=GROUPS), :]

        def chunk(n, prev):
            finish(*prev)
            begin(p, n)
            return p, n

        return lax.fori_loop(0, p // CHUNK + 1, chunk, prev)

    finish(*lax.fori_loop(0, DATES, covariances, (jnp.int32(0), jnp.int32(0))))

    ref = flipped(my_date, date_turns, ref_ref[0])

    def send(g):
        for off in range(1, devices):
            pltpu.make_async_remote_copy(
                src_ref=tile.at[g, off // per_date], dst_ref=o_ref.at[me, g],
                send_sem=sent.at[1], recv_sem=got_sem.at[0],
                device_id={"pix": peers[off]}, device_id_type=MESH,
            ).start()
        pltpu.make_async_copy(tile.at[g, 0], o_ref.at[me, g], local.at[6]).start()

    def solve(g, carry):
        for i in range(DATES):
            cov[g, i, i, 0] = cov[g, i, i, 0] + load[g]
        for i in range(DATES):
            one, two = jnp.maximum(ref, i), jnp.minimum(ref, i)
            real = cov[g, one, two, 0]
            imag = 0.5 * (cov[g, one, two, 1] + cov[g, one, two, 2])
            sign = jnp.where(ref == i, 0.0, jnp.where(ref < i, 1.0, -1.0))
            imag = imag * sign
            vec[0, i, 0] = real
            vec[0, i, 1] = imag
            vec[0, i, 2] = real + imag

        @pl.when(g > 0)
        def _():
            send(g - 1)

        def step(t, carry):
            src = lax.rem(t, 2)
            for base in range(0, DATES, SPAN):
                acc = [[None] * 3 for _ in range(SPAN)]
                for j in range(DATES):
                    vr, vi, vs = vec[src, j, 0], vec[src, j, 1], vec[src, j, 2]
                    for q in range(SPAN):
                        i = base + q
                        one, two = max(i, j), min(i, j)
                        cr = cov[g, one, two, 0]
                        if i == j:
                            terms, minus = (None, cr * vr, cr * vi), (False, True, False)
                        elif i > j:
                            terms = (cr * vs, cov[g, i, j, 1] * vi, cov[g, i, j, 2] * vr)
                            minus = (False, False, False)
                        else:
                            terms = (cr * vs, cov[g, j, i, 2] * vi, cov[g, j, i, 1] * vr)
                            minus = (False, True, True)
                        for n in range(3):
                            if terms[n] is None:
                                continue
                            if acc[q][n] is None:
                                acc[q][n] = -terms[n] if minus[n] else terms[n]
                            elif minus[n]:
                                acc[q][n] = acc[q][n] - terms[n]
                            else:
                                acc[q][n] = acc[q][n] + terms[n]
                for q in range(SPAN):
                    real, imag = acc[q][0] - acc[q][1], acc[q][0] + acc[q][2]
                    vec[1 - src, base + q, 0] = real
                    vec[1 - src, base + q, 1] = imag
                    vec[1 - src, base + q, 2] = real + imag
            return carry

        lax.fori_loop(0, POWER_ITERS - 1, step, 0)
        last = (POWER_ITERS - 1) % 2
        total = jnp.zeros((SUB, columns), f32)
        for k in range(DATES):
            vr, vi = vec[last, k, 0], vec[last, k, 1]
            total = total + (vr * vr + vi * vi)
        scale = DATES / total
        rr, ri = vec[last, ref, 0] * scale, vec[last, ref, 1] * scale
        comp_r = jnp.zeros_like(total)
        comp_i = jnp.zeros_like(total)
        at = pl.ds(pl.multiple_of(g * SUB, SUB), SUB)
        for k in range(DATES):
            vr, vi = vec[last, k, 0], vec[last, k, 1]
            lr = vr * rr + vi * ri
            li = vi * rr - vr * ri
            zr, zi = zb[k, 0, at], zb[k, 1, at]
            comp_r = comp_r + (lr * zr + li * zi)
            comp_i = comp_i + (lr * zi - li * zr)
            tile[g, k] = jnp.concatenate([lr, li], axis=0).astype(bf16)
        comp[0, g] = comp_r * (1.0 / math.sqrt(DATES))
        comp[1, g] = comp_i * (1.0 / math.sqrt(DATES))
        return carry

    lax.fori_loop(0, GROUPS, solve, 0)
    pltpu.make_async_remote_copy(
        src_ref=win.at[0:devices - 1], dst_ref=win.at[0:devices - 1], send_sem=sent.at[0],
        recv_sem=rsem.at[0], device_id={"pix": peers[1]}, device_id_type=MESH,
    ).wait_send()
    send(GROUPS - 1)
    out = pltpu.make_async_copy(comp, comp_ref, local.at[7])
    out.start()
    pltpu.make_async_copy(tile.at[:, 0], o_ref.at[me], local.at[6]).wait()
    out.wait()
    others = o_ref.at[0:devices - 1]
    pltpu.make_async_remote_copy(
        src_ref=others, dst_ref=others, send_sem=sent.at[1], recv_sem=got_sem.at[0],
        device_id={"pix": peers[1]}, device_id_type=MESH,
    ).wait()


def spectrum_kernel(got_ref, table_ref, comp_ref, o_ref, out_ref, got, table, comp, order, out, ins, outs):
    devices, columns = got.shape[0], got.shape[3]
    local_rows = out.shape[1]
    parts = outs.shape[0] - 1
    size = devices // parts

    def copy_in(n):
        at = pl.ds(n * size, size)
        return pltpu.make_async_copy(got_ref.at[at], got.at[at], ins.at[n])

    def copy_out(n):
        at = pl.ds(n * size * columns, size * columns)
        return pltpu.make_async_copy(out.at[:, :, at], o_ref.at[:, :, at], outs.at[n])

    tables = pltpu.make_async_copy(table_ref, table, ins.at[parts])
    comps = pltpu.make_async_copy(comp_ref, comp, ins.at[parts + 1])
    tables.start()
    for n in range(parts):
        copy_in(n).start()
    comps.start()
    tables.wait()
    for n in range(parts):
        copy_in(n).wait()
        for m in range(0, size, 2):
            at = n * size + m
            both = jnp.concatenate(
                [got[at].reshape(2 * ROWS, columns), got[at + 1].reshape(2 * ROWS, columns)], axis=1
            )
            value = jnp.dot(
                table[...], jnp.concatenate([both, both], axis=0), preferred_element_type=jnp.float32
            )
            for c in range(2):
                out[c, :, at * columns:(at + 2) * columns] = value[c * local_rows:(c + 1) * local_rows]
        copy_out(n).start()
    comps.wait()
    for c in range(2):
        for g in range(GROUPS):
            order[c, pl.ds(g, SUB, stride=GROUPS), :] = comp[c, g]
    last = pltpu.make_async_copy(order, out_ref, outs.at[parts])
    last.start()
    for n in range(parts):
        copy_out(n).wait()
    last.wait()


def on_device(slcs, ref_date):
    devices = lax.axis_size("pix")
    local_rows, strip_columns = slcs.shape[1], slcs.shape[2]
    columns = strip_columns // devices
    per_date = ROWS // local_rows

    anywhere = pl.BlockSpec(memory_space=pl.ANY)
    both, pick, order = window_weights(columns), pick_weights(columns), order_weights(local_rows)
    mask = block_masks()
    table = dct_weights(local_rows)
    f32, bf16 = jnp.float32, jnp.bfloat16
    phases, compressed = pl.pallas_call(
        functools.partial(link_kernel, devices),
        out_shape=(
            jax.ShapeDtypeStruct((devices, GROUPS, 2 * SUB, columns), bf16),
            jax.ShapeDtypeStruct((2, GROUPS, SUB, columns), f32),
        ),
        in_specs=[pl.BlockSpec(memory_space=pltpu.SMEM)] + [anywhere] * 5,
        out_specs=(anywhere, anywhere),
        scratch_shapes=[
            pltpu.VMEM((2 * local_rows, strip_columns + 2 * columns), bf16),
            pltpu.VMEM((devices, 2 * local_rows + HALO, columns), bf16),
            pltpu.VMEM((devices, HALO, LANES), bf16),
            pltpu.VMEM((DATES // PACK, 2, ROWS, LANES), f32),
            pltpu.VMEM((2, ROWS, LANES), f32),
            pltpu.VMEM(both.shape, bf16),
            pltpu.VMEM(pick.shape, bf16),
            pltpu.VMEM(order.shape, bf16),
            pltpu.VMEM(mask.shape, f32),
            pltpu.VMEM((2, ROWS, columns), f32),
            pltpu.VMEM((DATES, 2, ROWS, columns), f32),
            pltpu.VMEM((2 * CHUNK * ROWS, columns), f32),
            pltpu.VMEM((GROUPS, SUB, columns), f32),
            pltpu.VMEM((GROUPS, DATES, DATES, 3, SUB, columns), f32),
            pltpu.VMEM((2, DATES, 3, SUB, columns), f32),
            pltpu.VMEM((GROUPS, DATES, 2 * SUB, columns), bf16),
            pltpu.VMEM((2, GROUPS, SUB, columns), f32),
            pltpu.SemaphoreType.DMA((8,)),
            pltpu.SemaphoreType.DMA((2,)),
            pltpu.SemaphoreType.DMA((devices,)),
            pltpu.SemaphoreType.DMA((1,)),
        ],
        compiler_params=pltpu.CompilerParams(
            collective_id=0, has_side_effects=True, vmem_limit_bytes=60 * 1024 * 1024
        ),
        name="link",
    )(ref_date, slcs.reshape(2 * local_rows, strip_columns), both, pick, order, mask)

    if per_date > 1:
        table = lax.dynamic_index_in_dim(table, lax.rem(lax.axis_index("pix"), per_date), 0, False)
    else:
        table = table[0]
    parts = 2
    return pl.pallas_call(
        spectrum_kernel,
        out_shape=(
            jax.ShapeDtypeStruct((2, local_rows, strip_columns), f32),
            jax.ShapeDtypeStruct((2, ROWS, columns), f32),
        ),
        in_specs=[anywhere] * 3,
        out_specs=(anywhere, anywhere),
        scratch_shapes=[
            pltpu.VMEM((devices, GROUPS, 2 * SUB, columns), bf16),
            pltpu.VMEM(table.shape, bf16),
            pltpu.VMEM((2, GROUPS, SUB, columns), f32),
            pltpu.VMEM((2, ROWS, columns), f32),
            pltpu.VMEM((2, local_rows, strip_columns), f32),
            pltpu.SemaphoreType.DMA((parts + 2,)),
            pltpu.SemaphoreType.DMA((parts + 1,)),
        ],
        name="spectrum",
    )(phases, table, compressed)


def solution(mesh):
    return jax.shard_map(
        on_device,
        mesh=mesh,
        in_specs=(P(None, ("grp", "pix"), None), P("grp")),
        out_specs=(P(None, ("grp", "pix"), None), P(None, None, ("grp", "pix"))),
        check_vma=False,
    )
```

```python
import functools
import math

import jax
import jax.numpy as jnp
import numpy as np
from jax import lax
from jax.experimental import pallas as pl
from jax.experimental.pallas import tpu as pltpu
from jax.sharding import PartitionSpec as P

DATES = 16
ROWS = 64
HALF_X = 5
HALF_Y = 2
POWER_ITERS = 6
LOADING = 0.25

LANES = 128
SUB = 8
GROUPS = ROWS // SUB
HALO = 16
PACK = LANES // HALO
CHUNK = 8
BATCH = 2
SPAN = 8
SCALE = 2.0 ** -6
LINK_VMEM = 40 * 1024 * 1024
SPECTRUM_VMEM = 12 * 1024 * 1024
MESH = pl.DeviceIdType.MESH


def window_weights(columns):
    target = np.arange(columns)[None, :]
    band = np.abs(np.arange(columns)[:, None] - target) <= HALF_X
    outside = np.concatenate([np.arange(-HALF_X, 0), columns + np.arange(HALF_X)])
    halo = np.zeros((HALO, columns), np.float32)
    halo[: 2 * HALF_X] = np.abs(outside[:, None] - target) <= HALF_X
    both = np.concatenate([band.astype(np.float32), np.tile(halo, (PACK, 1))], axis=0)
    return jnp.asarray(both * SCALE, jnp.bfloat16)


def pick_weights(columns):
    pick = np.zeros((HALO, 2 * columns), np.float32)
    for h in range(HALF_X):
        pick[h, columns - HALF_X + h] = 1.0
        pick[HALF_X + h, columns + h] = 1.0
    return jnp.asarray(pick, jnp.bfloat16)


def order_weights(local_rows):
    per_date = ROWS // local_rows
    order = np.zeros((2, GROUPS, SUB, per_date, LANES), np.float32)
    for c in range(2):
        for line in range(ROWS):
            q, r = divmod(line, local_rows)
            order[c, line % GROUPS, line // GROUPS, q, c * local_rows + r] = 1.0
    return jnp.asarray(order.reshape(2 * ROWS, per_date * LANES), jnp.bfloat16)


def block_masks():
    block = np.arange(PACK)[:, None, None] == (np.arange(LANES) // HALO)[None, None, :]
    return jnp.asarray(np.broadcast_to(block, (PACK, 2 * SUB, LANES)), jnp.float32)


def dct_weights(local_rows):
    frequency = np.arange(ROWS, dtype=np.float64)[:, None]
    position = np.arange(ROWS, dtype=np.float64)[None, :]
    weight = np.where(frequency == 0, math.sqrt(1.0 / ROWS), math.sqrt(2.0 / ROWS))
    table = weight * np.cos(np.pi * (2.0 * position + 1.0) * frequency / (2.0 * ROWS))
    table = table.reshape(ROWS // local_rows, local_rows, SUB, GROUPS).transpose(0, 1, 3, 2)
    big = np.zeros((ROWS // local_rows, 2, local_rows, GROUPS, 2, SUB), np.float32)
    for c in range(2):
        big[:, c, :, :, c] = table
    big = big.reshape(ROWS // local_rows, 2 * local_rows, 2 * ROWS)
    high = big.astype(jnp.bfloat16)
    low = (big - high.astype(np.float32)).astype(jnp.bfloat16)
    return jnp.asarray(np.concatenate([high, low], axis=2))


def pair_products(one, two):
    real = one[0] * two[0] + one[1] * two[1]
    imag = one[1] * two[0] - one[0] * two[1]
    return real, imag


def tall_of(value, rows):
    return jnp.concatenate([value] * (rows // value.shape[0]), axis=0)


def flips(a, size):
    out, bit = [], 1
    while bit < size:
        out.append(bit - 2 * bit * ((a // bit) % 2))
        bit *= 2
    return out


def flipped(a, deltas, b):
    for n, delta in enumerate(deltas):
        if isinstance(b, int):
            a = a + delta if (b >> n) & 1 else a
        else:
            a = a + delta * ((b // (1 << n)) % 2)
    return a


def link_kernel(devices, ref_ref, x_ref, both_ref, pick_ref, order_ref, mask_ref,
                o_ref, comp_ref,
                xs, win, hsend, edge, wide, both, pick, order, mask,
                stage, zb, summed, load, cov, vec, tile, comp,
                local, sent, rsem, got_sem):
    columns = win.shape[2]
    height = x_ref.shape[0]
    local_rows = height // 2
    strip_columns = x_ref.shape[1]
    per_date = ROWS // local_rows
    me = lax.axis_index("pix")
    my_date = me // per_date
    turns = flips(me, devices)
    date_turns = turns[(per_date - 1).bit_length():]
    peers = [flipped(me, turns, off) for off in range(devices)]
    bf16, f32 = jnp.bfloat16, jnp.float32

    barrier = pltpu.get_barrier_semaphore()
    for peer in peers[1:]:
        pl.semaphore_signal(barrier, inc=1, device_id={"pix": peer}, device_id_type=MESH)

    def block(n):
        return x_ref.at[:, pl.ds(pl.multiple_of(n * columns, columns), columns)]

    loads = [
        pltpu.make_async_copy(src, dst, local.at[n])
        for n, (src, dst) in enumerate((
            (x_ref, xs.at[:, columns:columns + strip_columns]),
            (pick_ref, pick), (block(me), win.at[me, 0:height]), (both_ref, both), (order_ref, order),
            (mask_ref, mask),
        ))
    ]
    for copy in loads:
        copy.start()

    def main_copy(off, peer):
        return pltpu.make_async_remote_copy(
            src_ref=block(peer), dst_ref=win.at[me, 0:height], send_sem=sent.at[0],
            recv_sem=rsem.at[off], device_id={"pix": peer}, device_id_type=MESH,
        )

    def halo_copy(off, peer):
        return pltpu.make_async_remote_copy(
            src_ref=hsend.at[peer], dst_ref=win.at[me, height:height + HALO], send_sem=sent.at[0],
            recv_sem=rsem.at[off], device_id={"pix": peer}, device_id_type=MESH,
        )

    quarter = devices // 4
    first = sorted({1, 2, 3, quarter, quarter + 1, 2 * quarter, 2 * quarter + 1})
    later = [off for off in range(1, devices) if off not in first]
    halos = [halo_copy(off, peers[off]) for off in range(1, devices)]
    mains = {off: main_copy(off, peers[off]) for off in range(1, devices)}

    pl.semaphore_wait(barrier, devices - 1)
    for off in first:
        mains[off].start()

    margin = jnp.zeros((height, columns), bf16)
    xs[:, 0:columns] = margin
    xs[:, columns + strip_columns:2 * columns + strip_columns] = margin
    loads[0].wait()
    loads[1].wait()

    blocks = min(devices, 16)

    def cut_halos(n, carry):
        for q in range(blocks):
            at = (n * blocks + q) * columns
            left = xs[:, pl.ds(pl.multiple_of(at, columns), columns)]
            right = xs[:, pl.ds(pl.multiple_of(at + 2 * columns, columns), columns)]
            near = jnp.concatenate([left, right], axis=1)
            if height < LANES:
                fill = jnp.zeros((LANES - height, 2 * columns), bf16)
                near = jnp.concatenate([near, fill], axis=0)
            got = lax.dot_general(
                pick[...], near, (((1,), (1,)), ((), ())), preferred_element_type=f32
            )
            hsend[n * blocks + q] = got.astype(bf16)
        return carry

    lax.fori_loop(0, devices // blocks, cut_halos, 0)
    win[me, height:height + HALO] = hsend[me]
    for c in halos:
        c.start()
    for off in later:
        mains[off].start()

    first_column = me * columns
    sub = lax.broadcasted_iota(jnp.int32, (SUB, columns), 0)
    lane = lax.broadcasted_iota(jnp.int32, (SUB, columns), 1) + first_column
    across = jnp.minimum(lane + HALF_X, strip_columns - 1) - jnp.maximum(lane - HALF_X, 0) + 1
    for g in range(GROUPS):
        line = sub * GROUPS + g
        along = jnp.minimum(line + HALF_Y, ROWS - 1) - jnp.maximum(line - HALF_Y, 0) + 1
        load[g] = (along * across).astype(f32) * (LOADING * SCALE)
    edge[...] = jnp.zeros_like(edge)
    for copy in loads[2:]:
        copy.wait()

    def date_at(p):
        return flipped(my_date, date_turns, p)

    def tall(value):
        return tall_of(value, ROWS)

    def window_sums(plane):
        rows = [plane[g * SUB:(g + 1) * SUB] for g in range(GROUPS)]
        before = [jnp.where(sub == 0, 0.0, pltpu.roll(x, 1, 0)) for x in rows[-HALF_Y:]]
        after = [jnp.where(sub == SUB - 1, 0.0, pltpu.roll(x, SUB - 1, 0)) for x in rows[:HALF_Y]]
        ext = before + rows + after
        two = [ext[2 * k] + ext[2 * k + 1] for k in range(GROUPS // 2 + 2)]
        four = [two[k] + two[k + 1] for k in range(GROUPS // 2 + 1)]
        out = []
        for k in range(GROUPS // 2):
            out.append(four[k] + ext[2 * k + 4])
            out.append(ext[2 * k + 1] + four[k + 1])
        return out

    def finish(b, n):
        for d in range(BATCH):
            p = b * BATCH + d
            for q in range(CHUNK):
                first_row = (d * CHUNK + q) * 2 * ROWS
                sums = [
                    window_sums(summed[first_row + part * ROWS:first_row + (part + 1) * ROWS])
                    for part in range(2)
                ]
                for g in range(GROUPS):
                    real, imag = sums[0][g], sums[1][g]
                    cov[g, p, n * CHUNK + q, 0] = real
                    cov[g, p, n * CHUNK + q, 1] = real + imag
                    cov[g, p, n * CHUNK + q, 2] = imag - real

    def begin(b, n):
        half = (n * CHUNK) // PACK
        planes = []
        beside = edge[half, 0].astype(bf16), edge[half, 1].astype(bf16)
        for d in range(BATCH):
            p = b * BATCH + d
            one = zb[p, 0].astype(bf16), zb[p, 1].astype(bf16)
            margins = pair_products((wide[d, 0].astype(bf16), wide[d, 1].astype(bf16)), beside)
            for q in range(CHUNK):
                k = n * CHUNK + q
                two = zb[k, 0].astype(bf16), zb[k, 1].astype(bf16)
                keep = tall(mask[k - half * PACK].astype(bf16))
                for value, margin in zip(pair_products(one, two), margins):
                    planes.append(jnp.concatenate([value, margin * keep], axis=1))
        summed[...] = jnp.dot(
            jnp.concatenate(planes, axis=0), both[...], preferred_element_type=f32
        )

    def covariances(b, prev):
        for n in range(BATCH * per_date):
            off = b * (BATCH * per_date) + n
            source = flipped(me, turns, off)

            @pl.when(off != 0)
            def _():
                pltpu.make_async_remote_copy(
                    src_ref=win.at[source], dst_ref=win.at[source], send_sem=sent.at[0],
                    recv_sem=rsem.at[off], device_id={"pix": source}, device_id_type=MESH,
                ).wait_recv()

        for d in range(BATCH):
            p = b * BATCH + d
            sources = [date_at(p) * per_date + q for q in range(per_date)]
            margin = jnp.concatenate(
                [tall_of(win[source, height:height + HALO], LANES) for source in sources], axis=1
            )
            got = lax.dot_general(
                order[...], margin, (((1,), (1,)), ((), ())), preferred_element_type=f32
            )
            keep = tall(mask[lax.rem(p, PACK)])
            half = p // PACK
            for c in range(2):
                part = got[c * ROWS:(c + 1) * ROWS]
                wide[d, c] = part
                edge[half, c] = edge[half, c] + part * keep
            for q, source in enumerate(sources):
                for c in range(2):
                    stage[d, c, q * local_rows:(q + 1) * local_rows] = win[
                        source, c * local_rows:(c + 1) * local_rows
                    ].astype(f32)
            for c in range(2):
                for g in range(GROUPS):
                    zb[p, c, g * SUB:(g + 1) * SUB] = stage[d, c, pl.ds(g, SUB, stride=GROUPS), :]

        def chunk(n, prev):
            finish(*prev)
            begin(b, n)
            return b, n

        return lax.fori_loop(0, (b * BATCH + BATCH - 1) // CHUNK + 1, chunk, prev)

    finish(*lax.fori_loop(0, DATES // BATCH, covariances, (jnp.int32(0), jnp.int32(0))))

    ref = flipped(my_date, date_turns, ref_ref[0])

    def send(g):
        for off in range(1, devices):
            pltpu.make_async_remote_copy(
                src_ref=tile.at[g, off // per_date], dst_ref=o_ref.at[me, g],
                send_sem=sent.at[1], recv_sem=got_sem.at[0],
                device_id={"pix": peers[off]}, device_id_type=MESH,
            ).start()
        pltpu.make_async_copy(tile.at[g, 0], o_ref.at[me, g], local.at[6]).start()

    def solve(g, carry):
        for i in range(DATES):
            cov[g, i, i, 0] = cov[g, i, i, 0] + load[g]
        for i in range(DATES):
            one, two = jnp.maximum(ref, i), jnp.minimum(ref, i)
            real = cov[g, one, two, 0]
            imag = 0.5 * (cov[g, one, two, 1] + cov[g, one, two, 2])
            sign = jnp.where(ref == i, 0.0, jnp.where(ref < i, 1.0, -1.0))
            imag = imag * sign
            vec[0, i, 0] = real
            vec[0, i, 1] = imag
            vec[0, i, 2] = real + imag

        @pl.when(g > 0)
        def _():
            send(g - 1)

        def step(t, carry):
            src = lax.rem(t, 2)
            for base in range(0, DATES, SPAN):
                acc = [[None] * 3 for _ in range(SPAN)]
                for j in range(DATES):
                    vr, vi, vs = vec[src, j, 0], vec[src, j, 1], vec[src, j, 2]
                    for q in range(SPAN):
                        i = base + q
                        one, two = max(i, j), min(i, j)
                        cr = cov[g, one, two, 0]
                        if i == j:
                            terms, minus = (None, cr * vr, cr * vi), (False, True, False)
                        elif i > j:
                            terms = (cr * vs, cov[g, i, j, 1] * vi, cov[g, i, j, 2] * vr)
                            minus = (False, False, False)
                        else:
                            terms = (cr * vs, cov[g, j, i, 2] * vi, cov[g, j, i, 1] * vr)
                            minus = (False, True, True)
                        for n in range(3):
                            if terms[n] is None:
                                continue
                            if acc[q][n] is None:
                                acc[q][n] = -terms[n] if minus[n] else terms[n]
                            elif minus[n]:
                                acc[q][n] = acc[q][n] - terms[n]
                            else:
                                acc[q][n] = acc[q][n] + terms[n]
                for q in range(SPAN):
                    real, imag = acc[q][0] - acc[q][1], acc[q][0] + acc[q][2]
                    vec[1 - src, base + q, 0] = real
                    vec[1 - src, base + q, 1] = imag
                    vec[1 - src, base + q, 2] = real + imag
            return carry

        lax.fori_loop(0, POWER_ITERS - 1, step, 0)
        last = (POWER_ITERS - 1) % 2
        total = jnp.zeros((SUB, columns), f32)
        for k in range(DATES):
            vr, vi = vec[last, k, 0], vec[last, k, 1]
            total = total + (vr * vr + vi * vi)
        scale = DATES / total
        rr, ri = vec[last, ref, 0] * scale, vec[last, ref, 1] * scale
        comp_r = jnp.zeros_like(total)
        comp_i = jnp.zeros_like(total)
        at = pl.ds(pl.multiple_of(g * SUB, SUB), SUB)
        for k in range(DATES):
            vr, vi = vec[last, k, 0], vec[last, k, 1]
            lr = vr * rr + vi * ri
            li = vi * rr - vr * ri
            zr, zi = zb[k, 0, at], zb[k, 1, at]
            comp_r = comp_r + (lr * zr + li * zi)
            comp_i = comp_i + (lr * zi - li * zr)
            tile[g, k] = jnp.concatenate([lr, li], axis=0).astype(bf16)
        comp[0, g] = comp_r * (1.0 / math.sqrt(DATES))
        comp[1, g] = comp_i * (1.0 / math.sqrt(DATES))
        return carry

    lax.fori_loop(0, GROUPS, solve, 0)
    pltpu.make_async_remote_copy(
        src_ref=win.at[0:devices - 1], dst_ref=win.at[0:devices - 1], send_sem=sent.at[0],
        recv_sem=rsem.at[0], device_id={"pix": peers[1]}, device_id_type=MESH,
    ).wait_send()
    send(GROUPS - 1)
    out = pltpu.make_async_copy(comp, comp_ref, local.at[7])
    out.start()
    pltpu.make_async_copy(tile.at[:, 0], o_ref.at[me], local.at[6]).wait()
    out.wait()
    others = o_ref.at[0:devices - 1]
    pltpu.make_async_remote_copy(
        src_ref=others, dst_ref=others, send_sem=sent.at[1], recv_sem=got_sem.at[0],
        device_id={"pix": peers[1]}, device_id_type=MESH,
    ).wait()


def spectrum_kernel(got, table, comp, o_ref, out_ref, order, out, outs):
    devices, columns = got.shape[0], got.shape[3]
    local_rows = out.shape[1]
    parts = outs.shape[0] - 1
    size = devices // parts

    def copy_out(n):
        at = pl.ds(n * size * columns, size * columns)
        return pltpu.make_async_copy(out.at[:, :, at], o_ref.at[:, :, at], outs.at[n])

    for c in range(2):
        for g in range(GROUPS):
            order[c, pl.ds(g, SUB, stride=GROUPS), :] = comp[c, g]
    last = pltpu.make_async_copy(order, out_ref, outs.at[parts])
    last.start()
    for n in range(parts):
        for m in range(0, size, 2):
            at = n * size + m
            both = jnp.concatenate(
                [got[at].reshape(2 * ROWS, columns), got[at + 1].reshape(2 * ROWS, columns)], axis=1
            )
            value = jnp.dot(
                table[...], jnp.concatenate([both, both], axis=0), preferred_element_type=jnp.float32
            )
            for c in range(2):
                out[c, :, at * columns:(at + 2) * columns] = value[c * local_rows:(c + 1) * local_rows]
        copy_out(n).start()
    for n in range(parts):
        copy_out(n).wait()
    last.wait()


def on_device(slcs, ref_date):
    devices = lax.axis_size("pix")
    local_rows, strip_columns = slcs.shape[1], slcs.shape[2]
    columns = strip_columns // devices
    per_date = ROWS // local_rows

    anywhere = pl.BlockSpec(memory_space=pl.ANY)
    hbm = pl.BlockSpec(memory_space=pltpu.HBM)
    vmem = pl.BlockSpec(memory_space=pltpu.VMEM)
    both, pick, order = window_weights(columns), pick_weights(columns), order_weights(local_rows)
    mask = block_masks()
    table = dct_weights(local_rows)
    f32, bf16 = jnp.float32, jnp.bfloat16
    phases, compressed = pl.pallas_call(
        functools.partial(link_kernel, devices),
        out_shape=(
            jax.ShapeDtypeStruct((devices, GROUPS, 2 * SUB, columns), bf16),
            jax.ShapeDtypeStruct((2, GROUPS, SUB, columns), f32),
        ),
        in_specs=[pl.BlockSpec(memory_space=pltpu.SMEM)] + [hbm] * 5,
        out_specs=(anywhere, anywhere),
        scratch_shapes=[
            pltpu.VMEM((2 * local_rows, strip_columns + 2 * columns), bf16),
            pltpu.VMEM((devices, 2 * local_rows + HALO, columns), bf16),
            pltpu.VMEM((devices, HALO, LANES), bf16),
            pltpu.VMEM((DATES // PACK, 2, ROWS, LANES), f32),
            pltpu.VMEM((BATCH, 2, ROWS, LANES), f32),
            pltpu.VMEM(both.shape, bf16),
            pltpu.VMEM(pick.shape, bf16),
            pltpu.VMEM(order.shape, bf16),
            pltpu.VMEM(mask.shape, f32),
            pltpu.VMEM((BATCH, 2, ROWS, columns), f32),
            pltpu.VMEM((DATES, 2, ROWS, columns), f32),
            pltpu.VMEM((2 * BATCH * CHUNK * ROWS, columns), f32),
            pltpu.VMEM((GROUPS, SUB, columns), f32),
            pltpu.VMEM((GROUPS, DATES, DATES, 3, SUB, columns), f32),
            pltpu.VMEM((2, DATES, 3, SUB, columns), f32),
            pltpu.VMEM((GROUPS, DATES, 2 * SUB, columns), bf16),
            pltpu.VMEM((2, GROUPS, SUB, columns), f32),
            pltpu.SemaphoreType.DMA((8,)),
            pltpu.SemaphoreType.DMA((2,)),
            pltpu.SemaphoreType.DMA((devices,)),
            pltpu.SemaphoreType.DMA((1,)),
        ],
        compiler_params=pltpu.CompilerParams(
            collective_id=0, has_side_effects=True, vmem_limit_bytes=LINK_VMEM
        ),
        name="link",
    )(
        ref_date,
        *(
            pltpu.with_memory_space_constraint(value, pltpu.HBM)
            for value in (slcs.reshape(2 * local_rows, strip_columns), both, pick, order, mask)
        ),
    )

    if per_date > 1:
        table = lax.dynamic_index_in_dim(table, lax.rem(lax.axis_index("pix"), per_date), 0, False)
    else:
        table = table[0]
    parts = 2
    return pl.pallas_call(
        spectrum_kernel,
        out_shape=(
            jax.ShapeDtypeStruct((2, local_rows, strip_columns), f32),
            jax.ShapeDtypeStruct((2, ROWS, columns), f32),
        ),
        in_specs=[vmem] * 3,
        out_specs=(hbm, hbm),
        scratch_shapes=[
            pltpu.VMEM((2, ROWS, columns), f32),
            pltpu.VMEM((2, local_rows, strip_columns), f32),
            pltpu.SemaphoreType.DMA((parts + 1,)),
        ],
        compiler_params=pltpu.CompilerParams(vmem_limit_bytes=SPECTRUM_VMEM),
        name="spectrum",
    )(phases, table, compressed)


def solution(mesh):
    return jax.shard_map(
        on_device,
        mesh=mesh,
        in_specs=(P(None, ("grp", "pix"), None), P("grp")),
        out_specs=(P(None, ("grp", "pix"), None), P(None, None, ("grp", "pix"))),
        check_vma=False,
    )
```

```python
import functools
import math

import jax
import jax.numpy as jnp
import numpy as np
from jax import lax
from jax.experimental import pallas as pl
from jax.experimental.pallas import tpu as pltpu
from jax.sharding import PartitionSpec as P

DATES = 16
ROWS = 64
HALF_X = 5
HALF_Y = 2
POWER_ITERS = 6
LOADING = 0.25

LANES = 128
SUB = 8
GROUPS = ROWS // SUB
HALO = 16
PACK = LANES // HALO
CHUNK = 8
BATCH = 2
ORDER = (0, 1, 2, 3, 4, 5, 6, 7)
FIRST = 10
ROUNDS = tuple((g, 1) for g in range(GROUPS))
SPAN = 8
SCALE = 2.0 ** -6
LINK_VMEM = 40 * 1024 * 1024
SPECTRUM_VMEM = 12 * 1024 * 1024
MESH = pl.DeviceIdType.MESH


def window_weights(columns):
    target = np.arange(columns)[None, :]
    band = np.abs(np.arange(columns)[:, None] - target) <= HALF_X
    outside = np.concatenate([np.arange(-HALF_X, 0), columns + np.arange(HALF_X)])
    halo = np.zeros((HALO, columns), np.float32)
    halo[: 2 * HALF_X] = np.abs(outside[:, None] - target) <= HALF_X
    both = np.concatenate([band.astype(np.float32), np.tile(halo, (PACK, 1))], axis=0)
    return jnp.asarray(both * SCALE, jnp.bfloat16)


def pick_weights(columns):
    pick = np.zeros((HALO, 2 * columns), np.float32)
    for h in range(HALF_X):
        pick[h, columns - HALF_X + h] = 1.0
        pick[HALF_X + h, columns + h] = 1.0
    return jnp.asarray(pick, jnp.bfloat16)


def order_weights(local_rows):
    per_date = ROWS // local_rows
    order = np.zeros((2, GROUPS, SUB, per_date, LANES), np.float32)
    for c in range(2):
        for line in range(ROWS):
            q, r = divmod(line, local_rows)
            order[c, line % GROUPS, line // GROUPS, q, c * local_rows + r] = 1.0
    return jnp.asarray(order.reshape(2 * ROWS, per_date * LANES), jnp.bfloat16)


def block_masks():
    block = np.arange(PACK)[:, None, None] == (np.arange(LANES) // HALO)[None, None, :]
    return jnp.asarray(np.broadcast_to(block, (PACK, 2 * SUB, LANES)), jnp.float32)


def dct_weights(local_rows):
    frequency = np.arange(ROWS, dtype=np.float64)[:, None]
    position = np.arange(ROWS, dtype=np.float64)[None, :]
    weight = np.where(frequency == 0, math.sqrt(1.0 / ROWS), math.sqrt(2.0 / ROWS))
    table = weight * np.cos(np.pi * (2.0 * position + 1.0) * frequency / (2.0 * ROWS))
    table = table.reshape(ROWS // local_rows, local_rows, SUB, GROUPS).transpose(0, 1, 3, 2)
    big = np.zeros((ROWS // local_rows, 2, local_rows, GROUPS, 2, SUB), np.float32)
    for c in range(2):
        big[:, c, :, :, c] = table
    big = big.reshape(ROWS // local_rows, 2 * local_rows, 2 * ROWS)
    high = big.astype(jnp.bfloat16)
    low = (big - high.astype(np.float32)).astype(jnp.bfloat16)
    return jnp.asarray(np.concatenate([high, low], axis=2))


def pair_products(one, two):
    real = one[0] * two[0] + one[1] * two[1]
    imag = one[1] * two[0] - one[0] * two[1]
    return real, imag


def tall_of(value, rows):
    return jnp.concatenate([value] * (rows // value.shape[0]), axis=0)


def flips(a, size):
    out, bit = [], 1
    while bit < size:
        out.append(bit - 2 * bit * ((a // bit) % 2))
        bit *= 2
    return out


def flipped(a, deltas, b):
    for n, delta in enumerate(deltas):
        if isinstance(b, int):
            a = a + delta if (b >> n) & 1 else a
        else:
            a = a + delta * ((b // (1 << n)) % 2)
    return a


def chosen(b):
    return sum(jnp.where(b == n, value, 0) for n, value in enumerate(ORDER))


def placed(b):
    return sum(jnp.where(b == value, n, 0) for n, value in enumerate(ORDER))


def link_kernel(devices, ref_ref, x_ref, both_ref, pick_ref, order_ref, mask_ref,
                o_ref, comp_ref,
                xs, win, hsend, edge, wide, both, pick, order, mask,
                stage, zb, summed, load, cov, vec, tile, comp,
                local, sent, rsem, got_sem):
    columns = win.shape[2]
    height = x_ref.shape[0]
    local_rows = height // 2
    strip_columns = x_ref.shape[1]
    per_date = ROWS // local_rows
    me = lax.axis_index("pix")
    my_date = me // per_date
    turns = flips(me, devices)
    date_turns = turns[(per_date - 1).bit_length():]
    peers = [flipped(me, turns, off) for off in range(devices)]
    bf16, f32 = jnp.bfloat16, jnp.float32

    barrier = pltpu.get_barrier_semaphore()
    for peer in peers[1:]:
        pl.semaphore_signal(barrier, inc=1, device_id={"pix": peer}, device_id_type=MESH)

    def block(n):
        return x_ref.at[:, pl.ds(pl.multiple_of(n * columns, columns), columns)]

    loads = [
        pltpu.make_async_copy(src, dst, local.at[n])
        for n, (src, dst) in enumerate((
            (x_ref, xs.at[:, columns:columns + strip_columns]),
            (pick_ref, pick), (block(me), win.at[me, 0:height]), (both_ref, both), (order_ref, order),
            (mask_ref, mask),
        ))
    ]
    for copy in loads:
        copy.start()

    def main_copy(off, peer):
        return pltpu.make_async_remote_copy(
            src_ref=block(peer), dst_ref=win.at[me, 0:height], send_sem=sent.at[0],
            recv_sem=rsem.at[off], device_id={"pix": peer}, device_id_type=MESH,
        )

    def halo_copy(off, peer):
        return pltpu.make_async_remote_copy(
            src_ref=hsend.at[peer], dst_ref=win.at[me, height:height + HALO], send_sem=sent.at[0],
            recv_sem=rsem.at[off], device_id={"pix": peer}, device_id_type=MESH,
        )

    queue = [o * BATCH * per_date + n for o in ORDER for n in range(BATCH * per_date)][1:]
    first, later = queue[:FIRST], queue[FIRST:]
    halos = [halo_copy(off, peers[off]) for off in queue]
    mains = {off: main_copy(off, peers[off]) for off in range(1, devices)}

    pl.semaphore_wait(barrier, devices - 1)
    for off in first:
        mains[off].start()

    margin = jnp.zeros((height, columns), bf16)
    xs[:, 0:columns] = margin
    xs[:, columns + strip_columns:2 * columns + strip_columns] = margin
    loads[0].wait()
    loads[1].wait()

    blocks = min(devices, 16)

    def cut_halos(n, carry):
        for q in range(blocks):
            at = (n * blocks + q) * columns
            left = xs[:, pl.ds(pl.multiple_of(at, columns), columns)]
            right = xs[:, pl.ds(pl.multiple_of(at + 2 * columns, columns), columns)]
            near = jnp.concatenate([left, right], axis=1)
            if height < LANES:
                fill = jnp.zeros((LANES - height, 2 * columns), bf16)
                near = jnp.concatenate([near, fill], axis=0)
            got = lax.dot_general(
                pick[...], near, (((1,), (1,)), ((), ())), preferred_element_type=f32
            )
            hsend[n * blocks + q] = got.astype(bf16)
        return carry

    lax.fori_loop(0, devices // blocks, cut_halos, 0)
    win[me, height:height + HALO] = hsend[me]
    for c in halos:
        c.start()
    for off in later:
        mains[off].start()

    first_column = me * columns
    sub = lax.broadcasted_iota(jnp.int32, (SUB, columns), 0)
    lane = lax.broadcasted_iota(jnp.int32, (SUB, columns), 1) + first_column
    across = jnp.minimum(lane + HALF_X, strip_columns - 1) - jnp.maximum(lane - HALF_X, 0) + 1
    for g in range(GROUPS):
        line = sub * GROUPS + g
        along = jnp.minimum(line + HALF_Y, ROWS - 1) - jnp.maximum(line - HALF_Y, 0) + 1
        load[g] = (along * across).astype(f32) * (LOADING * SCALE)
    edge[...] = jnp.zeros_like(edge)
    for copy in loads[2:]:
        copy.wait()

    def tall(value):
        return tall_of(value, ROWS)

    def window_sums(plane):
        rows = [plane[g * SUB:(g + 1) * SUB] for g in range(GROUPS)]
        before = [jnp.where(sub == 0, 0.0, pltpu.roll(x, 1, 0)) for x in rows[-HALF_Y:]]
        after = [jnp.where(sub == SUB - 1, 0.0, pltpu.roll(x, SUB - 1, 0)) for x in rows[:HALF_Y]]
        ext = before + rows + after
        two = [ext[2 * k] + ext[2 * k + 1] for k in range(GROUPS // 2 + 2)]
        four = [two[k] + two[k + 1] for k in range(GROUPS // 2 + 1)]
        out = []
        for k in range(GROUPS // 2):
            out.append(four[k] + ext[2 * k + 4])
            out.append(ext[2 * k + 1] + four[k + 1])
        return out

    def finish(b, n):
        for d in range(BATCH):
            p = b * BATCH + d
            for q in range(CHUNK):
                first_row = (d * CHUNK + q) * 2 * ROWS
                sums = [
                    window_sums(summed[first_row + part * ROWS:first_row + (part + 1) * ROWS])
                    for part in range(2)
                ]
                for g in range(GROUPS):
                    real, imag = sums[0][g], sums[1][g]
                    cov[g, p, n * CHUNK + q, 0] = real
                    cov[g, p, n * CHUNK + q, 1] = real + imag
                    cov[g, p, n * CHUNK + q, 2] = imag - real

    def diagonal(b, n):
        last = jnp.where(n == (b * BATCH + BATCH - 1) // CHUNK, 1.0, 0.0)
        for g in range(GROUPS):
            more = load[g] * last
            for d in range(BATCH):
                p = b * BATCH + d
                cov[g, p, p, 0] = cov[g, p, p, 0] + more

    def begin(b, n):
        half = (n * CHUNK) // PACK
        planes = []
        beside = edge[half, 0].astype(bf16), edge[half, 1].astype(bf16)
        for d in range(BATCH):
            p = b * BATCH + d
            one = zb[p, 0].astype(bf16), zb[p, 1].astype(bf16)
            margins = pair_products((wide[d, 0].astype(bf16), wide[d, 1].astype(bf16)), beside)
            for q in range(CHUNK):
                k = n * CHUNK + q
                two = zb[k, 0].astype(bf16), zb[k, 1].astype(bf16)
                keep = tall(mask[k - half * PACK].astype(bf16))
                for value, margin in zip(pair_products(one, two), margins):
                    planes.append(jnp.concatenate([value, margin * keep], axis=1))
        summed[...] = jnp.dot(
            jnp.concatenate(planes, axis=0), both[...], preferred_element_type=f32
        )

    def covariances(b, prev):
        pick_b = chosen(b)
        for n in range(BATCH * per_date):
            off = pick_b * (BATCH * per_date) + n
            source = flipped(me, turns, off)

            @pl.when(off != 0)
            def _():
                pltpu.make_async_remote_copy(
                    src_ref=win.at[source], dst_ref=win.at[source], send_sem=sent.at[0],
                    recv_sem=rsem.at[off], device_id={"pix": source}, device_id_type=MESH,
                ).wait_recv()

        for d in range(BATCH):
            p = b * BATCH + d
            date = flipped(my_date, date_turns, pick_b * BATCH + d)
            sources = [date * per_date + q for q in range(per_date)]
            margin = jnp.concatenate(
                [tall_of(win[source, height:height + HALO], LANES) for source in sources], axis=1
            )
            got = lax.dot_general(
                order[...], margin, (((1,), (1,)), ((), ())), preferred_element_type=f32
            )
            keep = tall(mask[lax.rem(p, PACK)])
            half = p // PACK
            for c in range(2):
                part = got[c * ROWS:(c + 1) * ROWS]
                wide[d, c] = part
                edge[half, c] = edge[half, c] + part * keep
            for q, source in enumerate(sources):
                for c in range(2):
                    stage[d, c, q * local_rows:(q + 1) * local_rows] = win[
                        source, c * local_rows:(c + 1) * local_rows
                    ].astype(f32)
            for c in range(2):
                for g in range(GROUPS):
                    zb[p, c, g * SUB:(g + 1) * SUB] = stage[d, c, pl.ds(g, SUB, stride=GROUPS), :]

        def chunk(n, prev):
            finish(*prev)
            diagonal(*prev)
            begin(b, n)
            return b, n

        return lax.fori_loop(0, (b * BATCH + BATCH - 1) // CHUNK + 1, chunk, prev)

    last = lax.fori_loop(0, DATES // BATCH, covariances, (jnp.int32(0), jnp.int32(0)))
    finish(*last)
    diagonal(*last)

    ref_off = flipped(my_date, date_turns, ref_ref[0])
    ref = placed(ref_off // BATCH) * BATCH + ref_off % BATCH
    places = [ORDER.index(n // BATCH) * BATCH + n % BATCH for n in range(DATES)]

    def send(g, size):
        at = pl.ds(g, size)
        for off in queue:
            pltpu.make_async_remote_copy(
                src_ref=tile.at[at, places[off // per_date]], dst_ref=o_ref.at[me, at],
                send_sem=sent.at[1], recv_sem=got_sem.at[0],
                device_id={"pix": peers[off]}, device_id_type=MESH,
            ).start()
        pltpu.make_async_copy(tile.at[at, 0], o_ref.at[me, at], local.at[6]).start()

    def solve(g, carry):
        for i in range(DATES):
            one, two = jnp.maximum(ref, i), jnp.minimum(ref, i)
            real = cov[g, one, two, 0]
            imag = 0.5 * (cov[g, one, two, 1] + cov[g, one, two, 2])
            sign = jnp.where(ref == i, 0.0, jnp.where(ref < i, 1.0, -1.0))
            imag = imag * sign
            vec[0, i, 0] = real
            vec[0, i, 1] = imag
            vec[0, i, 2] = real + imag

        for start, size in ROUNDS[:-1]:
            @pl.when(g == start + size)
            def _():
                send(start, size)

        def step(t):
            src = t % 2
            for base in range(0, DATES, SPAN):
                acc = [[None] * 3 for _ in range(SPAN)]
                for j in range(DATES):
                    vr, vi, vs = vec[src, j, 0], vec[src, j, 1], vec[src, j, 2]
                    for q in range(SPAN):
                        i = base + q
                        one, two = max(i, j), min(i, j)
                        cr = cov[g, one, two, 0]
                        if i == j:
                            terms, minus = (None, cr * vr, cr * vi), (False, True, False)
                        elif i > j:
                            terms = (cr * vs, cov[g, i, j, 1] * vi, cov[g, i, j, 2] * vr)
                            minus = (False, False, False)
                        else:
                            terms = (cr * vs, cov[g, j, i, 2] * vi, cov[g, j, i, 1] * vr)
                            minus = (False, True, True)
                        for n in range(3):
                            if terms[n] is None:
                                continue
                            if acc[q][n] is None:
                                acc[q][n] = -terms[n] if minus[n] else terms[n]
                            elif minus[n]:
                                acc[q][n] = acc[q][n] - terms[n]
                            else:
                                acc[q][n] = acc[q][n] + terms[n]
                for q in range(SPAN):
                    real, imag = acc[q][0] - acc[q][1], acc[q][0] + acc[q][2]
                    vec[1 - src, base + q, 0] = real
                    vec[1 - src, base + q, 1] = imag
                    vec[1 - src, base + q, 2] = real + imag

        for t in range(POWER_ITERS - 1):
            step(t)
        last = (POWER_ITERS - 1) % 2
        total = jnp.zeros((SUB, columns), f32)
        for k in range(DATES):
            vr, vi = vec[last, k, 0], vec[last, k, 1]
            total = total + (vr * vr + vi * vi)
        scale = DATES / total
        rr, ri = vec[last, ref, 0] * scale, vec[last, ref, 1] * scale
        comp_r = jnp.zeros_like(total)
        comp_i = jnp.zeros_like(total)
        at = pl.ds(pl.multiple_of(g * SUB, SUB), SUB)
        for k in range(DATES):
            vr, vi = vec[last, k, 0], vec[last, k, 1]
            lr = vr * rr + vi * ri
            li = vi * rr - vr * ri
            zr, zi = zb[k, 0, at], zb[k, 1, at]
            comp_r = comp_r + (lr * zr + li * zi)
            comp_i = comp_i + (lr * zi - li * zr)
            tile[g, k] = jnp.concatenate([lr, li], axis=0).astype(bf16)
        comp[0, g] = comp_r * (1.0 / math.sqrt(DATES))
        comp[1, g] = comp_i * (1.0 / math.sqrt(DATES))
        return carry

    lax.fori_loop(0, GROUPS, solve, 0)
    pltpu.make_async_remote_copy(
        src_ref=win.at[0:devices - 1], dst_ref=win.at[0:devices - 1], send_sem=sent.at[0],
        recv_sem=rsem.at[0], device_id={"pix": peers[1]}, device_id_type=MESH,
    ).wait_send()
    send(*ROUNDS[-1])
    out = pltpu.make_async_copy(comp, comp_ref, local.at[7])
    out.start()
    pltpu.make_async_copy(tile.at[:, 0], o_ref.at[me], local.at[6]).wait()
    out.wait()
    others = o_ref.at[0:devices - 1]
    pltpu.make_async_remote_copy(
        src_ref=others, dst_ref=others, send_sem=sent.at[1], recv_sem=got_sem.at[0],
        device_id={"pix": peers[1]}, device_id_type=MESH,
    ).wait()


def spectrum_kernel(got, table, comp, o_ref, out_ref, order, out, outs):
    devices, columns = got.shape[0], got.shape[3]
    local_rows = out.shape[1]
    parts = outs.shape[0] - 1
    size = devices // parts

    def copy_out(n):
        at = pl.ds(n * size * columns, size * columns)
        return pltpu.make_async_copy(out.at[:, :, at], o_ref.at[:, :, at], outs.at[n])

    for c in range(2):
        for g in range(GROUPS):
            order[c, pl.ds(g, SUB, stride=GROUPS), :] = comp[c, g]
    last = pltpu.make_async_copy(order, out_ref, outs.at[parts])
    last.start()
    for n in range(parts):
        for m in range(0, size, 2):
            at = n * size + m
            both = jnp.concatenate(
                [got[at].reshape(2 * ROWS, columns), got[at + 1].reshape(2 * ROWS, columns)], axis=1
            )
            value = jnp.dot(
                table[...], jnp.concatenate([both, both], axis=0), preferred_element_type=jnp.float32
            )
            for c in range(2):
                out[c, :, at * columns:(at + 2) * columns] = value[c * local_rows:(c + 1) * local_rows]
        copy_out(n).start()
    for n in range(parts):
        copy_out(n).wait()
    last.wait()


def on_device(slcs, ref_date):
    devices = lax.axis_size("pix")
    local_rows, strip_columns = slcs.shape[1], slcs.shape[2]
    columns = strip_columns // devices
    per_date = ROWS // local_rows

    anywhere = pl.BlockSpec(memory_space=pl.ANY)
    hbm = pl.BlockSpec(memory_space=pltpu.HBM)
    vmem = pl.BlockSpec(memory_space=pltpu.VMEM)
    both, pick, order = window_weights(columns), pick_weights(columns), order_weights(local_rows)
    mask = block_masks()
    table = dct_weights(local_rows)
    f32, bf16 = jnp.float32, jnp.bfloat16
    phases, compressed = pl.pallas_call(
        functools.partial(link_kernel, devices),
        out_shape=(
            jax.ShapeDtypeStruct((devices, GROUPS, 2 * SUB, columns), bf16),
            jax.ShapeDtypeStruct((2, GROUPS, SUB, columns), f32),
        ),
        in_specs=[pl.BlockSpec(memory_space=pltpu.SMEM)] + [hbm] * 5,
        out_specs=(anywhere, anywhere),
        scratch_shapes=[
            pltpu.VMEM((2 * local_rows, strip_columns + 2 * columns), bf16),
            pltpu.VMEM((devices, 2 * local_rows + HALO, columns), bf16),
            pltpu.VMEM((devices, HALO, LANES), bf16),
            pltpu.VMEM((DATES // PACK, 2, ROWS, LANES), f32),
            pltpu.VMEM((BATCH, 2, ROWS, LANES), f32),
            pltpu.VMEM(both.shape, bf16),
            pltpu.VMEM(pick.shape, bf16),
            pltpu.VMEM(order.shape, bf16),
            pltpu.VMEM(mask.shape, f32),
            pltpu.VMEM((BATCH, 2, ROWS, columns), f32),
            pltpu.VMEM((DATES, 2, ROWS, columns), f32),
            pltpu.VMEM((2 * BATCH * CHUNK * ROWS, columns), f32),
            pltpu.VMEM((GROUPS, SUB, columns), f32),
            pltpu.VMEM((GROUPS, DATES, DATES, 3, SUB, columns), f32),
            pltpu.VMEM((2, DATES, 3, SUB, columns), f32),
            pltpu.VMEM((GROUPS, DATES, 2 * SUB, columns), bf16),
            pltpu.VMEM((2, GROUPS, SUB, columns), f32),
            pltpu.SemaphoreType.DMA((8,)),
            pltpu.SemaphoreType.DMA((2,)),
            pltpu.SemaphoreType.DMA((devices,)),
            pltpu.SemaphoreType.DMA((1,)),
        ],
        compiler_params=pltpu.CompilerParams(
            collective_id=0, has_side_effects=True, vmem_limit_bytes=LINK_VMEM
        ),
        name="link",
    )(
        ref_date,
        *(
            pltpu.with_memory_space_constraint(value, pltpu.HBM)
            for value in (slcs.reshape(2 * local_rows, strip_columns), both, pick, order, mask)
        ),
    )

    if per_date > 1:
        table = lax.dynamic_index_in_dim(table, lax.rem(lax.axis_index("pix"), per_date), 0, False)
    else:
        table = table[0]
    parts = 4
    return pl.pallas_call(
        spectrum_kernel,
        out_shape=(
            jax.ShapeDtypeStruct((2, local_rows, strip_columns), f32),
            jax.ShapeDtypeStruct((2, ROWS, columns), f32),
        ),
        in_specs=[vmem] * 3,
        out_specs=(hbm, hbm),
        scratch_shapes=[
            pltpu.VMEM((2, ROWS, columns), f32),
            pltpu.VMEM((2, local_rows, strip_columns), f32),
            pltpu.SemaphoreType.DMA((parts + 1,)),
        ],
        compiler_params=pltpu.CompilerParams(vmem_limit_bytes=SPECTRUM_VMEM),
        name="spectrum",
    )(phases, table, compressed)


def solution(mesh):
    return jax.shard_map(
        on_device,
        mesh=mesh,
        in_specs=(P(None, ("grp", "pix"), None), P("grp")),
        out_specs=(P(None, ("grp", "pix"), None), P(None, None, ("grp", "pix"))),
        check_vma=False,
    )
```

```python
import functools
import math

import jax
import jax.numpy as jnp
import numpy as np
from jax import lax
from jax.experimental import pallas as pl
from jax.experimental.pallas import tpu as pltpu
from jax.sharding import PartitionSpec as P

DATES = 16
ROWS = 64
HALF_X = 5
HALF_Y = 2
POWER_ITERS = 6
LOADING = 0.25

LANES = 128
SUB = 8
GROUPS = ROWS // SUB
HALO = 16
EDGE = 2 * HALF_X
PACK = LANES // HALO
CHUNK = 8
BATCH = 2
ORDER = (0, 1, 2, 3, 4, 5, 6, 7)
FIRST = 10
SPAN = 8
SCALE = 2.0 ** -6
LINK_VMEM = 40 * 1024 * 1024
SPECTRUM_VMEM = 12 * 1024 * 1024
MESH = pl.DeviceIdType.MESH


def window_weights(columns):
    target = np.arange(columns)[None, :]
    band = np.abs(np.arange(columns)[:, None] - target) <= HALF_X
    outside = np.concatenate([np.arange(-HALF_X, 0), columns + np.arange(HALF_X)])
    halo = np.zeros((HALO, columns), np.float32)
    halo[: 2 * HALF_X] = np.abs(outside[:, None] - target) <= HALF_X
    both = np.concatenate([band.astype(np.float32), np.tile(halo, (PACK, 1))], axis=0)
    return jnp.asarray(both * SCALE, jnp.bfloat16)


def pick_weights(columns):
    pick = np.zeros((HALO, 2 * columns), np.float32)
    for h in range(HALF_X):
        pick[h, columns - HALF_X + h] = 1.0
        pick[HALF_X + h, columns + h] = 1.0
    return jnp.asarray(pick, jnp.bfloat16)


def order_weights(local_rows):
    per_date = ROWS // local_rows
    order = np.zeros((2, GROUPS, SUB, per_date, LANES), np.float32)
    for c in range(2):
        for line in range(ROWS):
            q, r = divmod(line, local_rows)
            order[c, line % GROUPS, line // GROUPS, q, c * local_rows + r] = 1.0
    return jnp.asarray(order.reshape(2 * ROWS, per_date * LANES), jnp.bfloat16)


def block_masks():
    block = np.arange(PACK)[:, None, None] == (np.arange(LANES) // HALO)[None, None, :]
    return jnp.asarray(np.broadcast_to(block, (PACK, 2 * SUB, LANES)), jnp.float32)


def dct_weights(local_rows):
    frequency = np.arange(ROWS, dtype=np.float64)[:, None]
    position = np.arange(ROWS, dtype=np.float64)[None, :]
    weight = np.where(frequency == 0, math.sqrt(1.0 / ROWS), math.sqrt(2.0 / ROWS))
    table = weight * np.cos(np.pi * (2.0 * position + 1.0) * frequency / (2.0 * ROWS))
    table = table.reshape(ROWS // local_rows, local_rows, SUB, GROUPS).transpose(0, 1, 3, 2)
    big = np.zeros((ROWS // local_rows, 2, local_rows, GROUPS, 2, SUB), np.float32)
    for c in range(2):
        big[:, c, :, :, c] = table
    big = big.reshape(ROWS // local_rows, 2 * local_rows, 2 * ROWS)
    high = big.astype(jnp.bfloat16)
    low = (big - high.astype(np.float32)).astype(jnp.bfloat16)
    return jnp.asarray(np.concatenate([high, low], axis=2))


def pair_products(one, two):
    real = one[0] * two[0] + one[1] * two[1]
    imag = one[1] * two[0] - one[0] * two[1]
    return real, imag


def tall_of(value, rows):
    return jnp.concatenate([value] * (rows // value.shape[0]), axis=0)


def flips(a, size):
    out, bit = [], 1
    while bit < size:
        out.append(bit - 2 * bit * ((a // bit) % 2))
        bit *= 2
    return out


def flipped(a, deltas, b):
    for n, delta in enumerate(deltas):
        if isinstance(b, int):
            a = a + delta if (b >> n) & 1 else a
        else:
            a = a + delta * ((b // (1 << n)) % 2)
    return a


def chosen(b):
    return sum(jnp.where(b == n, value, 0) for n, value in enumerate(ORDER))


def placed(b):
    return sum(jnp.where(b == value, n, 0) for n, value in enumerate(ORDER))


def link_kernel(devices, ref_ref, x_ref, both_ref, pick_ref, order_ref, mask_ref,
                o_ref, comp_ref,
                xs, win, hsend, hwin, edge, wide, both, pick, order, mask,
                stage, zb, summed, load, cov, vec, tile, comp,
                local, sent, rsem, hsem, got_sem):
    columns = win.shape[2]
    height = x_ref.shape[0]
    local_rows = height // 2
    strip_columns = x_ref.shape[1]
    per_date = ROWS // local_rows
    me = lax.axis_index("pix")
    my_date = me // per_date
    turns = flips(me, devices)
    date_turns = turns[(per_date - 1).bit_length():]
    peers = [flipped(me, turns, off) for off in range(devices)]
    bf16, f32 = jnp.bfloat16, jnp.float32

    barrier = pltpu.get_barrier_semaphore()
    for peer in peers[1:]:
        pl.semaphore_signal(barrier, inc=1, device_id={"pix": peer}, device_id_type=MESH)

    def block(n):
        return x_ref.at[:, pl.ds(pl.multiple_of(n * columns, columns), columns)]

    loads = [
        pltpu.make_async_copy(src, dst, local.at[n])
        for n, (src, dst) in enumerate((
            (x_ref, xs.at[:, columns:columns + strip_columns]),
            (pick_ref, pick), (block(me), win.at[me]), (both_ref, both), (order_ref, order),
            (mask_ref, mask),
        ))
    ]
    for copy in loads:
        copy.start()

    def main_copy(off, peer):
        return pltpu.make_async_remote_copy(
            src_ref=block(peer), dst_ref=win.at[me], send_sem=sent.at[0],
            recv_sem=rsem.at[off], device_id={"pix": peer}, device_id_type=MESH,
        )

    def halo_copy(off, peer):
        return pltpu.make_async_remote_copy(
            src_ref=hsend.at[peer], dst_ref=hwin.at[me], send_sem=sent.at[2],
            recv_sem=hsem.at[off], device_id={"pix": peer}, device_id_type=MESH,
        )

    queue = [o * BATCH * per_date + n for o in ORDER for n in range(BATCH * per_date)][1:]
    first, later = queue[:FIRST], queue[FIRST:]
    halos = [halo_copy(off, peers[off]) for off in queue]
    mains = {off: main_copy(off, peers[off]) for off in range(1, devices)}

    pl.semaphore_wait(barrier, devices - 1)
    for off in first:
        mains[off].start()

    margin = jnp.zeros((height, columns), bf16)
    xs[:, 0:columns] = margin
    xs[:, columns + strip_columns:2 * columns + strip_columns] = margin
    loads[0].wait()
    loads[1].wait()

    blocks = min(devices, 16)

    def cut_halos(n, carry):
        for q in range(blocks):
            at = (n * blocks + q) * columns
            left = xs[:, pl.ds(pl.multiple_of(at, columns), columns)]
            right = xs[:, pl.ds(pl.multiple_of(at + 2 * columns, columns), columns)]
            near = jnp.concatenate([left, right], axis=1)
            if height < LANES:
                fill = jnp.zeros((LANES - height, 2 * columns), bf16)
                near = jnp.concatenate([near, fill], axis=0)
            got = lax.dot_general(
                pick[...], near, (((1,), (1,)), ((), ())), preferred_element_type=f32
            )
            for r in range(EDGE // 2):
                hsend[n * blocks + q, r] = got[2 * r:2 * r + 2].astype(bf16)
        return carry

    lax.fori_loop(0, devices // blocks, cut_halos, 0)
    hwin[me] = hsend[me]
    for c in halos:
        c.start()
    for off in later:
        mains[off].start()

    first_column = me * columns
    sub = lax.broadcasted_iota(jnp.int32, (SUB, columns), 0)
    lane = lax.broadcasted_iota(jnp.int32, (SUB, columns), 1) + first_column
    across = jnp.minimum(lane + HALF_X, strip_columns - 1) - jnp.maximum(lane - HALF_X, 0) + 1
    for g in range(GROUPS):
        line = sub * GROUPS + g
        along = jnp.minimum(line + HALF_Y, ROWS - 1) - jnp.maximum(line - HALF_Y, 0) + 1
        load[g] = (along * across).astype(f32) * (LOADING * SCALE)
    edge[...] = jnp.zeros_like(edge)
    for copy in loads[2:]:
        copy.wait()

    def tall(value):
        return tall_of(value, ROWS)

    def window_sums(plane):
        rows = [plane[g * SUB:(g + 1) * SUB] for g in range(GROUPS)]
        before = [jnp.where(sub == 0, 0.0, pltpu.roll(x, 1, 0)) for x in rows[-HALF_Y:]]
        after = [jnp.where(sub == SUB - 1, 0.0, pltpu.roll(x, SUB - 1, 0)) for x in rows[:HALF_Y]]
        ext = before + rows + after
        two = [ext[2 * k] + ext[2 * k + 1] for k in range(GROUPS // 2 + 2)]
        four = [two[k] + two[k + 1] for k in range(GROUPS // 2 + 1)]
        out = []
        for k in range(GROUPS // 2):
            out.append(four[k] + ext[2 * k + 4])
            out.append(ext[2 * k + 1] + four[k + 1])
        return out

    def finish(b, n):
        for d in range(BATCH):
            p = b * BATCH + d
            for q in range(CHUNK):
                first_row = (d * CHUNK + q) * 2 * ROWS
                sums = [
                    window_sums(summed[first_row + part * ROWS:first_row + (part + 1) * ROWS])
                    for part in range(2)
                ]
                for g in range(GROUPS):
                    real, imag = sums[0][g], sums[1][g]
                    cov[g, p, n * CHUNK + q, 0] = real
                    cov[g, p, n * CHUNK + q, 1] = real + imag
                    cov[g, p, n * CHUNK + q, 2] = imag - real

    def diagonal(b, n):
        last = jnp.where(n == (b * BATCH + BATCH - 1) // CHUNK, 1.0, 0.0)
        for g in range(GROUPS):
            more = load[g] * last
            for d in range(BATCH):
                p = b * BATCH + d
                cov[g, p, p, 0] = cov[g, p, p, 0] + more

    def begin(b, n):
        half = (n * CHUNK) // PACK
        planes = []
        beside = edge[half, 0].astype(bf16), edge[half, 1].astype(bf16)
        for d in range(BATCH):
            p = b * BATCH + d
            one = zb[p, 0].astype(bf16), zb[p, 1].astype(bf16)
            margins = pair_products((wide[d, 0].astype(bf16), wide[d, 1].astype(bf16)), beside)
            for q in range(CHUNK):
                k = n * CHUNK + q
                two = zb[k, 0].astype(bf16), zb[k, 1].astype(bf16)
                keep = tall(mask[k - half * PACK].astype(bf16))
                for value, margin in zip(pair_products(one, two), margins):
                    planes.append(jnp.concatenate([value, margin * keep], axis=1))
        summed[...] = jnp.dot(
            jnp.concatenate(planes, axis=0), both[...], preferred_element_type=f32
        )

    def rows_of(ref, source):
        rows = [ref[source, r].astype(f32) for r in range(EDGE // 2)]
        return jnp.concatenate(rows + [jnp.zeros((HALO - EDGE, LANES), f32)], axis=0).astype(bf16)

    def covariances(b, prev):
        pick_b = chosen(b)
        for n in range(BATCH * per_date):
            off = pick_b * (BATCH * per_date) + n
            source = flipped(me, turns, off)

            @pl.when(off != 0)
            def _():
                pltpu.make_async_remote_copy(
                    src_ref=hwin.at[source], dst_ref=hwin.at[source], send_sem=sent.at[2],
                    recv_sem=hsem.at[off], device_id={"pix": source}, device_id_type=MESH,
                ).wait_recv()
                pltpu.make_async_remote_copy(
                    src_ref=win.at[source], dst_ref=win.at[source], send_sem=sent.at[0],
                    recv_sem=rsem.at[off], device_id={"pix": source}, device_id_type=MESH,
                ).wait_recv()

        for d in range(BATCH):
            p = b * BATCH + d
            date = flipped(my_date, date_turns, pick_b * BATCH + d)
            sources = [date * per_date + q for q in range(per_date)]
            margin = jnp.concatenate(
                [tall_of(rows_of(hwin, source), LANES) for source in sources], axis=1
            )
            got = lax.dot_general(
                order[...], margin, (((1,), (1,)), ((), ())), preferred_element_type=f32
            )
            keep = tall(mask[lax.rem(p, PACK)])
            half = p // PACK
            for c in range(2):
                part = got[c * ROWS:(c + 1) * ROWS]
                wide[d, c] = part
                edge[half, c] = edge[half, c] + part * keep
            for q, source in enumerate(sources):
                for c in range(2):
                    stage[d, c, q * local_rows:(q + 1) * local_rows] = win[
                        source, c * local_rows:(c + 1) * local_rows
                    ].astype(f32)
            for c in range(2):
                for g in range(GROUPS):
                    zb[p, c, g * SUB:(g + 1) * SUB] = stage[d, c, pl.ds(g, SUB, stride=GROUPS), :]

        def chunk(n, prev):
            finish(*prev)
            diagonal(*prev)
            begin(b, n)
            return b, n

        return lax.fori_loop(0, (b * BATCH + BATCH - 1) // CHUNK + 1, chunk, prev)

    last = lax.fori_loop(0, DATES // BATCH, covariances, (jnp.int32(0), jnp.int32(0)))
    finish(*last)
    diagonal(*last)

    ref_off = flipped(my_date, date_turns, ref_ref[0])
    ref = placed(ref_off // BATCH) * BATCH + ref_off % BATCH
    places = [ORDER.index(n // BATCH) * BATCH + n % BATCH for n in range(DATES)]

    def send(g):
        for off in queue:
            pltpu.make_async_remote_copy(
                src_ref=tile.at[g, places[off // per_date]], dst_ref=o_ref.at[me, g],
                send_sem=sent.at[1], recv_sem=got_sem.at[0],
                device_id={"pix": peers[off]}, device_id_type=MESH,
            ).start()
        pltpu.make_async_copy(tile.at[g, 0], o_ref.at[me, g], local.at[6]).start()

    def solve(g, carry):
        for i in range(DATES):
            one, two = jnp.maximum(ref, i), jnp.minimum(ref, i)
            real = cov[g, one, two, 0]
            imag = 0.5 * (cov[g, one, two, 1] + cov[g, one, two, 2])
            sign = jnp.where(ref == i, 0.0, jnp.where(ref < i, 1.0, -1.0))
            imag = imag * sign
            vec[0, i, 0] = real
            vec[0, i, 1] = imag
            vec[0, i, 2] = real + imag

        @pl.when(g > 0)
        def _():
            send(g - 1)

        def step(t):
            src = t % 2
            for base in range(0, DATES, SPAN):
                acc = [[None] * 3 for _ in range(SPAN)]
                for j in range(DATES):
                    vr, vi, vs = vec[src, j, 0], vec[src, j, 1], vec[src, j, 2]
                    for q in range(SPAN):
                        i = base + q
                        one, two = max(i, j), min(i, j)
                        cr = cov[g, one, two, 0]
                        if i == j:
                            terms, minus = (None, cr * vr, cr * vi), (False, True, False)
                        elif i > j:
                            terms = (cr * vs, cov[g, i, j, 1] * vi, cov[g, i, j, 2] * vr)
                            minus = (False, False, False)
                        else:
                            terms = (cr * vs, cov[g, j, i, 2] * vi, cov[g, j, i, 1] * vr)
                            minus = (False, True, True)
                        for n in range(3):
                            if terms[n] is None:
                                continue
                            if acc[q][n] is None:
                                acc[q][n] = -terms[n] if minus[n] else terms[n]
                            elif minus[n]:
                                acc[q][n] = acc[q][n] - terms[n]
                            else:
                                acc[q][n] = acc[q][n] + terms[n]
                for q in range(SPAN):
                    real, imag = acc[q][0] - acc[q][1], acc[q][0] + acc[q][2]
                    vec[1 - src, base + q, 0] = real
                    vec[1 - src, base + q, 1] = imag
                    vec[1 - src, base + q, 2] = real + imag

        for t in range(POWER_ITERS - 1):
            step(t)
        last = (POWER_ITERS - 1) % 2
        total = jnp.zeros((SUB, columns), f32)
        for k in range(DATES):
            vr, vi = vec[last, k, 0], vec[last, k, 1]
            total = total + (vr * vr + vi * vi)
        scale = DATES / total
        rr, ri = vec[last, ref, 0] * scale, vec[last, ref, 1] * scale
        comp_r = jnp.zeros_like(total)
        comp_i = jnp.zeros_like(total)
        at = pl.ds(pl.multiple_of(g * SUB, SUB), SUB)
        for k in range(DATES):
            vr, vi = vec[last, k, 0], vec[last, k, 1]
            lr = vr * rr + vi * ri
            li = vi * rr - vr * ri
            zr, zi = zb[k, 0, at], zb[k, 1, at]
            comp_r = comp_r + (lr * zr + li * zi)
            comp_i = comp_i + (lr * zi - li * zr)
            tile[g, k] = jnp.concatenate([lr, li], axis=0).astype(bf16)
        comp[0, g] = comp_r * (1.0 / math.sqrt(DATES))
        comp[1, g] = comp_i * (1.0 / math.sqrt(DATES))
        return carry

    lax.fori_loop(0, GROUPS, solve, 0)
    pltpu.make_async_remote_copy(
        src_ref=win.at[0:devices - 1], dst_ref=win.at[0:devices - 1], send_sem=sent.at[0],
        recv_sem=rsem.at[0], device_id={"pix": peers[1]}, device_id_type=MESH,
    ).wait_send()
    pltpu.make_async_remote_copy(
        src_ref=hwin.at[0:devices - 1], dst_ref=hwin.at[0:devices - 1], send_sem=sent.at[2],
        recv_sem=hsem.at[0], device_id={"pix": peers[1]}, device_id_type=MESH,
    ).wait_send()
    send(GROUPS - 1)
    out = pltpu.make_async_copy(comp, comp_ref, local.at[7])
    out.start()
    pltpu.make_async_copy(tile.at[:, 0], o_ref.at[me], local.at[6]).wait()
    out.wait()
    others = o_ref.at[0:devices - 1]
    pltpu.make_async_remote_copy(
        src_ref=others, dst_ref=others, send_sem=sent.at[1], recv_sem=got_sem.at[0],
        device_id={"pix": peers[1]}, device_id_type=MESH,
    ).wait()


def spectrum_kernel(got, table, comp, o_ref, out_ref, order, out, outs):
    devices, columns = got.shape[0], got.shape[3]
    local_rows = out.shape[1]
    parts = outs.shape[0] - 1
    size = devices // parts

    def copy_out(n):
        at = pl.ds(n * size * columns, size * columns)
        return pltpu.make_async_copy(out.at[:, :, at], o_ref.at[:, :, at], outs.at[n])

    for c in range(2):
        for g in range(GROUPS):
            order[c, pl.ds(g, SUB, stride=GROUPS), :] = comp[c, g]
    last = pltpu.make_async_copy(order, out_ref, outs.at[parts])
    last.start()
    for n in range(parts):
        for m in range(0, size, 2):
            at = n * size + m
            both = jnp.concatenate(
                [got[at].reshape(2 * ROWS, columns), got[at + 1].reshape(2 * ROWS, columns)], axis=1
            )
            value = jnp.dot(
                table[...], jnp.concatenate([both, both], axis=0), preferred_element_type=jnp.float32
            )
            for c in range(2):
                out[c, :, at * columns:(at + 2) * columns] = value[c * local_rows:(c + 1) * local_rows]
        copy_out(n).start()
    for n in range(parts):
        copy_out(n).wait()
    last.wait()


def on_device(slcs, ref_date):
    devices = lax.axis_size("pix")
    local_rows, strip_columns = slcs.shape[1], slcs.shape[2]
    columns = strip_columns // devices
    per_date = ROWS // local_rows

    anywhere = pl.BlockSpec(memory_space=pl.ANY)
    hbm = pl.BlockSpec(memory_space=pltpu.HBM)
    vmem = pl.BlockSpec(memory_space=pltpu.VMEM)
    both, pick, order = window_weights(columns), pick_weights(columns), order_weights(local_rows)
    mask = block_masks()
    table = dct_weights(local_rows)
    f32, bf16 = jnp.float32, jnp.bfloat16
    phases, compressed = pl.pallas_call(
        functools.partial(link_kernel, devices),
        out_shape=(
            jax.ShapeDtypeStruct((devices, GROUPS, 2 * SUB, columns), bf16),
            jax.ShapeDtypeStruct((2, GROUPS, SUB, columns), f32),
        ),
        in_specs=[pl.BlockSpec(memory_space=pltpu.SMEM)] + [hbm] * 5,
        out_specs=(anywhere, anywhere),
        scratch_shapes=[
            pltpu.VMEM((2 * local_rows, strip_columns + 2 * columns), bf16),
            pltpu.VMEM((devices, 2 * local_rows, columns), bf16),
            pltpu.VMEM((devices, EDGE // 2, 2, LANES), bf16),
            pltpu.VMEM((devices, EDGE // 2, 2, LANES), bf16),
            pltpu.VMEM((DATES // PACK, 2, ROWS, LANES), f32),
            pltpu.VMEM((BATCH, 2, ROWS, LANES), f32),
            pltpu.VMEM(both.shape, bf16),
            pltpu.VMEM(pick.shape, bf16),
            pltpu.VMEM(order.shape, bf16),
            pltpu.VMEM(mask.shape, f32),
            pltpu.VMEM((BATCH, 2, ROWS, columns), f32),
            pltpu.VMEM((DATES, 2, ROWS, columns), f32),
            pltpu.VMEM((2 * BATCH * CHUNK * ROWS, columns), f32),
            pltpu.VMEM((GROUPS, SUB, columns), f32),
            pltpu.VMEM((GROUPS, DATES, DATES, 3, SUB, columns), f32),
            pltpu.VMEM((2, DATES, 3, SUB, columns), f32),
            pltpu.VMEM((GROUPS, DATES, 2 * SUB, columns), bf16),
            pltpu.VMEM((2, GROUPS, SUB, columns), f32),
            pltpu.SemaphoreType.DMA((8,)),
            pltpu.SemaphoreType.DMA((3,)),
            pltpu.SemaphoreType.DMA((devices,)),
            pltpu.SemaphoreType.DMA((devices,)),
            pltpu.SemaphoreType.DMA((1,)),
        ],
        compiler_params=pltpu.CompilerParams(
            collective_id=0, has_side_effects=True, vmem_limit_bytes=LINK_VMEM
        ),
        name="link",
    )(
        ref_date,
        *(
            pltpu.with_memory_space_constraint(value, pltpu.HBM)
            for value in (slcs.reshape(2 * local_rows, strip_columns), both, pick, order, mask)
        ),
    )

    if per_date > 1:
        table = lax.dynamic_index_in_dim(table, lax.rem(lax.axis_index("pix"), per_date), 0, False)
    else:
        table = table[0]
    parts = 4
    return pl.pallas_call(
        spectrum_kernel,
        out_shape=(
            jax.ShapeDtypeStruct((2, local_rows, strip_columns), f32),
            jax.ShapeDtypeStruct((2, ROWS, columns), f32),
        ),
        in_specs=[vmem] * 3,
        out_specs=(hbm, hbm),
        scratch_shapes=[
            pltpu.VMEM((2, ROWS, columns), f32),
            pltpu.VMEM((2, local_rows, strip_columns), f32),
            pltpu.SemaphoreType.DMA((parts + 1,)),
        ],
        compiler_params=pltpu.CompilerParams(vmem_limit_bytes=SPECTRUM_VMEM),
        name="spectrum",
    )(phases, table, compressed)


def solution(mesh):
    return jax.shard_map(
        on_device,
        mesh=mesh,
        in_specs=(P(None, ("grp", "pix"), None), P("grp")),
        out_specs=(P(None, ("grp", "pix"), None), P(None, None, ("grp", "pix"))),
        check_vma=False,
    )
```

```python
import functools
import math

import jax
import jax.numpy as jnp
import numpy as np
from jax import lax
from jax.experimental import pallas as pl
from jax.experimental.pallas import tpu as pltpu
from jax.sharding import PartitionSpec as P

DATES = 16
ROWS = 64
HALF_X = 5
HALF_Y = 2
POWER_ITERS = 6
LOADING = 0.25

LANES = 128
SUB = 8
GROUPS = ROWS // SUB
HALO = 16
EDGE = 2 * HALF_X
PACK = LANES // HALO
CHUNK = 8
BATCH = 2
FIRST = 10
SPAN = 8
SCALE = 2.0 ** -6
LINK_VMEM = 40 * 1024 * 1024
SPECTRUM_VMEM = 12 * 1024 * 1024
MESH = pl.DeviceIdType.MESH


def window_weights(columns):
    target = np.arange(columns)[None, :]
    band = np.abs(np.arange(columns)[:, None] - target) <= HALF_X
    outside = np.concatenate([np.arange(-HALF_X, 0), columns + np.arange(HALF_X)])
    halo = np.zeros((HALO, columns), np.float32)
    halo[: 2 * HALF_X] = np.abs(outside[:, None] - target) <= HALF_X
    both = np.concatenate([band.astype(np.float32), np.tile(halo, (PACK, 1))], axis=0)
    return jnp.asarray(both * SCALE, jnp.bfloat16)


def pick_weights(columns):
    pick = np.zeros((HALO, 2 * columns), np.float32)
    for h in range(HALF_X):
        pick[h, columns - HALF_X + h] = 1.0
        pick[HALF_X + h, columns + h] = 1.0
    return jnp.asarray(pick, jnp.bfloat16)


def order_weights(local_rows):
    per_date = ROWS // local_rows
    order = np.zeros((2, GROUPS, SUB, per_date, LANES), np.float32)
    for c in range(2):
        for line in range(ROWS):
            q, r = divmod(line, local_rows)
            order[c, line % GROUPS, line // GROUPS, q, c * local_rows + r] = 1.0
    return jnp.asarray(order.reshape(2 * ROWS, per_date * LANES), jnp.bfloat16)


def block_masks():
    block = np.arange(PACK)[:, None, None] == (np.arange(LANES) // HALO)[None, None, :]
    return jnp.asarray(np.broadcast_to(block, (PACK, 2 * SUB, LANES)), jnp.float32)


def dct_weights(local_rows):
    frequency = np.arange(ROWS, dtype=np.float64)[:, None]
    position = np.arange(ROWS, dtype=np.float64)[None, :]
    weight = np.where(frequency == 0, math.sqrt(1.0 / ROWS), math.sqrt(2.0 / ROWS))
    table = weight * np.cos(np.pi * (2.0 * position + 1.0) * frequency / (2.0 * ROWS))
    table = table.reshape(ROWS // local_rows, local_rows, SUB, GROUPS).transpose(0, 1, 3, 2)
    big = np.zeros((ROWS // local_rows, 2, local_rows, GROUPS, 2, SUB), np.float32)
    for c in range(2):
        big[:, c, :, :, c] = table
    big = big.reshape(ROWS // local_rows, 2 * local_rows, 2 * ROWS)
    high = big.astype(jnp.bfloat16)
    low = (big - high.astype(np.float32)).astype(jnp.bfloat16)
    return jnp.asarray(np.concatenate([high, low], axis=2))


def pair_products(one, two):
    real = one[0] * two[0] + one[1] * two[1]
    imag = one[1] * two[0] - one[0] * two[1]
    return real, imag


def tall_of(value, rows):
    return jnp.concatenate([value] * (rows // value.shape[0]), axis=0)


def flips(a, size):
    out, bit = [], 1
    while bit < size:
        out.append(bit - 2 * bit * ((a // bit) % 2))
        bit *= 2
    return out


def flipped(a, deltas, b):
    for n, delta in enumerate(deltas):
        if isinstance(b, int):
            a = a + delta if (b >> n) & 1 else a
        else:
            a = a + delta * ((b // (1 << n)) % 2)
    return a


def link_kernel(devices, ref_ref, x_ref, both_ref, pick_ref, order_ref, mask_ref,
                o_ref, comp_ref,
                xs, win, hsend, hwin, edge, wide, both, pick, order, mask,
                stage, zb, summed, load, cov, vec, tile, comp,
                local, sent, rsem, hsem, got_sem):
    columns = win.shape[2]
    height = x_ref.shape[0]
    local_rows = height // 2
    strip_columns = x_ref.shape[1]
    per_date = ROWS // local_rows
    me = lax.axis_index("pix")
    my_date = me // per_date
    turns = flips(me, devices)
    date_turns = turns[(per_date - 1).bit_length():]
    peers = [flipped(me, turns, off) for off in range(devices)]
    bf16, f32 = jnp.bfloat16, jnp.float32

    barrier = pltpu.get_barrier_semaphore()
    for peer in peers[1:]:
        pl.semaphore_signal(barrier, inc=1, device_id={"pix": peer}, device_id_type=MESH)

    def block(n):
        return x_ref.at[:, pl.ds(pl.multiple_of(n * columns, columns), columns)]

    loads = [
        pltpu.make_async_copy(src, dst, local.at[n])
        for n, (src, dst) in enumerate((
            (x_ref, xs.at[:, columns:columns + strip_columns]),
            (pick_ref, pick), (block(me), win.at[me]), (both_ref, both), (order_ref, order),
            (mask_ref, mask),
        ))
    ]
    for copy in loads:
        copy.start()

    def main_copy(off, peer):
        return pltpu.make_async_remote_copy(
            src_ref=block(peer), dst_ref=win.at[me], send_sem=sent.at[0],
            recv_sem=rsem.at[off], device_id={"pix": peer}, device_id_type=MESH,
        )

    def halo_copy(off, peer):
        return pltpu.make_async_remote_copy(
            src_ref=hsend.at[peer], dst_ref=hwin.at[me], send_sem=sent.at[2],
            recv_sem=hsem.at[off], device_id={"pix": peer}, device_id_type=MESH,
        )

    queue = list(range(1, devices))
    first, later = queue[:FIRST], queue[FIRST:]
    halos = [halo_copy(off, peers[off]) for off in queue]
    mains = {off: main_copy(off, peers[off]) for off in range(1, devices)}

    pl.semaphore_wait(barrier, devices - 1)
    for off in first:
        mains[off].start()

    margin = jnp.zeros((height, columns), bf16)
    xs[:, 0:columns] = margin
    xs[:, columns + strip_columns:2 * columns + strip_columns] = margin
    loads[0].wait()
    loads[1].wait()

    blocks = min(devices, 16)

    def cut_halos(n, carry):
        for q in range(blocks):
            at = (n * blocks + q) * columns
            left = xs[:, pl.ds(pl.multiple_of(at, columns), columns)]
            right = xs[:, pl.ds(pl.multiple_of(at + 2 * columns, columns), columns)]
            near = jnp.concatenate([left, right], axis=1)
            if height < LANES:
                fill = jnp.zeros((LANES - height, 2 * columns), bf16)
                near = jnp.concatenate([near, fill], axis=0)
            got = lax.dot_general(
                pick[...], near, (((1,), (1,)), ((), ())), preferred_element_type=f32
            )
            for r in range(EDGE // 2):
                hsend[n * blocks + q, r] = got[2 * r:2 * r + 2].astype(bf16)
        return carry

    lax.fori_loop(0, devices // blocks, cut_halos, 0)
    hwin[me] = hsend[me]
    for c in halos:
        c.start()
    for off in later:
        mains[off].start()

    first_column = me * columns
    sub = lax.broadcasted_iota(jnp.int32, (SUB, columns), 0)
    lane = lax.broadcasted_iota(jnp.int32, (SUB, columns), 1) + first_column
    across = jnp.minimum(lane + HALF_X, strip_columns - 1) - jnp.maximum(lane - HALF_X, 0) + 1
    for g in range(GROUPS):
        line = sub * GROUPS + g
        along = jnp.minimum(line + HALF_Y, ROWS - 1) - jnp.maximum(line - HALF_Y, 0) + 1
        load[g] = (along * across).astype(f32) * (LOADING * SCALE)
    edge[...] = jnp.zeros_like(edge)
    for copy in loads[2:]:
        copy.wait()

    def tall(value):
        return tall_of(value, ROWS)

    def window_sums(plane):
        rows = [plane[g * SUB:(g + 1) * SUB] for g in range(GROUPS)]
        before = [jnp.where(sub == 0, 0.0, pltpu.roll(x, 1, 0)) for x in rows[-HALF_Y:]]
        after = [jnp.where(sub == SUB - 1, 0.0, pltpu.roll(x, SUB - 1, 0)) for x in rows[:HALF_Y]]
        ext = before + rows + after
        two = [ext[2 * k] + ext[2 * k + 1] for k in range(GROUPS // 2 + 2)]
        four = [two[k] + two[k + 1] for k in range(GROUPS // 2 + 1)]
        out = []
        for k in range(GROUPS // 2):
            out.append(four[k] + ext[2 * k + 4])
            out.append(ext[2 * k + 1] + four[k + 1])
        return out

    def finish(b, n):
        for d in range(BATCH):
            p = b * BATCH + d
            for q in range(CHUNK):
                first_row = (d * CHUNK + q) * 2 * ROWS
                sums = [
                    window_sums(summed[first_row + part * ROWS:first_row + (part + 1) * ROWS])
                    for part in range(2)
                ]
                for g in range(GROUPS):
                    real, imag = sums[0][g], sums[1][g]
                    cov[g, p, n * CHUNK + q, 0] = real
                    cov[g, p, n * CHUNK + q, 1] = real + imag
                    cov[g, p, n * CHUNK + q, 2] = imag - real

    def diagonal(b, n):
        last = jnp.where(n == (b * BATCH + BATCH - 1) // CHUNK, 1.0, 0.0)
        for g in range(GROUPS):
            more = load[g] * last
            for d in range(BATCH):
                p = b * BATCH + d
                cov[g, p, p, 0] = cov[g, p, p, 0] + more

    def begin(b, n):
        half = (n * CHUNK) // PACK
        planes = []
        beside = edge[half, 0].astype(bf16), edge[half, 1].astype(bf16)
        for d in range(BATCH):
            p = b * BATCH + d
            one = zb[p, 0].astype(bf16), zb[p, 1].astype(bf16)
            margins = pair_products((wide[d, 0].astype(bf16), wide[d, 1].astype(bf16)), beside)
            for q in range(CHUNK):
                k = n * CHUNK + q
                two = zb[k, 0].astype(bf16), zb[k, 1].astype(bf16)
                keep = tall(mask[k - half * PACK].astype(bf16))
                for value, margin in zip(pair_products(one, two), margins):
                    planes.append(jnp.concatenate([value, margin * keep], axis=1))
        summed[...] = jnp.dot(
            jnp.concatenate(planes, axis=0), both[...], preferred_element_type=f32
        )

    def rows_of(ref, source):
        rows = [ref[source, r].astype(f32) for r in range(EDGE // 2)]
        return jnp.concatenate(rows + [jnp.zeros((HALO - EDGE, LANES), f32)], axis=0).astype(bf16)

    def covariances(b, prev):
        for n in range(BATCH * per_date):
            off = b * (BATCH * per_date) + n
            source = flipped(me, turns, off)

            @pl.when(off != 0)
            def _():
                pltpu.make_async_remote_copy(
                    src_ref=hwin.at[source], dst_ref=hwin.at[source], send_sem=sent.at[2],
                    recv_sem=hsem.at[off], device_id={"pix": source}, device_id_type=MESH,
                ).wait_recv()
                pltpu.make_async_remote_copy(
                    src_ref=win.at[source], dst_ref=win.at[source], send_sem=sent.at[0],
                    recv_sem=rsem.at[off], device_id={"pix": source}, device_id_type=MESH,
                ).wait_recv()

        for d in range(BATCH):
            p = b * BATCH + d
            date = flipped(my_date, date_turns, p)
            sources = [date * per_date + q for q in range(per_date)]
            margin = jnp.concatenate(
                [tall_of(rows_of(hwin, source), LANES) for source in sources], axis=1
            )
            got = lax.dot_general(
                order[...], margin, (((1,), (1,)), ((), ())), preferred_element_type=f32
            )
            keep = tall(mask[lax.rem(p, PACK)])
            half = p // PACK
            for c in range(2):
                part = got[c * ROWS:(c + 1) * ROWS]
                wide[d, c] = part
                edge[half, c] = edge[half, c] + part * keep
            for q, source in enumerate(sources):
                for c in range(2):
                    stage[d, c, q * local_rows:(q + 1) * local_rows] = win[
                        source, c * local_rows:(c + 1) * local_rows
                    ].astype(f32)
            for c in range(2):
                for g in range(GROUPS):
                    zb[p, c, g * SUB:(g + 1) * SUB] = stage[d, c, pl.ds(g, SUB, stride=GROUPS), :]

        def chunk(n, prev):
            finish(*prev)
            diagonal(*prev)
            begin(b, n)
            return b, n

        return lax.fori_loop(0, (b * BATCH + BATCH - 1) // CHUNK + 1, chunk, prev)

    last = lax.fori_loop(0, DATES // BATCH, covariances, (jnp.int32(0), jnp.int32(0)))
    finish(*last)
    diagonal(*last)

    ref = flipped(my_date, date_turns, ref_ref[0])

    def send(g):
        for off in queue:
            pltpu.make_async_remote_copy(
                src_ref=tile.at[g, off // per_date], dst_ref=o_ref.at[me, g],
                send_sem=sent.at[1], recv_sem=got_sem.at[0],
                device_id={"pix": peers[off]}, device_id_type=MESH,
            ).start()
        pltpu.make_async_copy(tile.at[g, 0], o_ref.at[me, g], local.at[6]).start()

    column = [
        (
            jnp.maximum(ref, i), jnp.minimum(ref, i),
            jnp.where(ref == i, 0.0, jnp.where(ref < i, 0.5, -0.5)),
        )
        for i in range(DATES)
    ]

    def solve(g, carry):
        for i, (one, two, sign) in enumerate(column):
            real = cov[g, one, two, 0]
            imag = (cov[g, one, two, 1] + cov[g, one, two, 2]) * sign
            vec[0, i, 0] = real
            vec[0, i, 1] = imag
            vec[0, i, 2] = real + imag

        @pl.when(g > 0)
        def _():
            send(g - 1)

        def step(t):
            src = t % 2
            for base in range(0, DATES, SPAN):
                acc = [[None] * 3 for _ in range(SPAN)]
                for j in range(DATES):
                    vr, vi, vs = vec[src, j, 0], vec[src, j, 1], vec[src, j, 2]
                    for q in range(SPAN):
                        i = base + q
                        one, two = max(i, j), min(i, j)
                        cr = cov[g, one, two, 0]
                        if i == j:
                            terms, minus = (None, cr * vr, cr * vi), (False, True, False)
                        elif i > j:
                            terms = (cr * vs, cov[g, i, j, 1] * vi, cov[g, i, j, 2] * vr)
                            minus = (False, False, False)
                        else:
                            terms = (cr * vs, cov[g, j, i, 2] * vi, cov[g, j, i, 1] * vr)
                            minus = (False, True, True)
                        for n in range(3):
                            if terms[n] is None:
                                continue
                            if acc[q][n] is None:
                                acc[q][n] = -terms[n] if minus[n] else terms[n]
                            elif minus[n]:
                                acc[q][n] = acc[q][n] - terms[n]
                            else:
                                acc[q][n] = acc[q][n] + terms[n]
                for q in range(SPAN):
                    real, imag = acc[q][0] - acc[q][1], acc[q][0] + acc[q][2]
                    vec[1 - src, base + q, 0] = real
                    vec[1 - src, base + q, 1] = imag
                    vec[1 - src, base + q, 2] = real + imag

        for t in range(POWER_ITERS - 1):
            step(t)
        last = (POWER_ITERS - 1) % 2
        total = jnp.zeros((SUB, columns), f32)
        for k in range(DATES):
            vr, vi = vec[last, k, 0], vec[last, k, 1]
            total = total + (vr * vr + vi * vi)
        scale = DATES / total
        rr, ri = vec[last, ref, 0] * scale, vec[last, ref, 1] * scale
        comp_r = jnp.zeros_like(total)
        comp_i = jnp.zeros_like(total)
        at = pl.ds(pl.multiple_of(g * SUB, SUB), SUB)
        for k in range(DATES):
            vr, vi = vec[last, k, 0], vec[last, k, 1]
            lr = vr * rr + vi * ri
            li = vi * rr - vr * ri
            zr, zi = zb[k, 0, at], zb[k, 1, at]
            comp_r = comp_r + (lr * zr + li * zi)
            comp_i = comp_i + (lr * zi - li * zr)
            tile[g, k] = jnp.concatenate([lr, li], axis=0).astype(bf16)
        comp[0, g] = comp_r * (1.0 / math.sqrt(DATES))
        comp[1, g] = comp_i * (1.0 / math.sqrt(DATES))
        return carry

    lax.fori_loop(0, GROUPS, solve, 0)
    pltpu.make_async_remote_copy(
        src_ref=win.at[0:devices - 1], dst_ref=win.at[0:devices - 1], send_sem=sent.at[0],
        recv_sem=rsem.at[0], device_id={"pix": peers[1]}, device_id_type=MESH,
    ).wait_send()
    pltpu.make_async_remote_copy(
        src_ref=hwin.at[0:devices - 1], dst_ref=hwin.at[0:devices - 1], send_sem=sent.at[2],
        recv_sem=hsem.at[0], device_id={"pix": peers[1]}, device_id_type=MESH,
    ).wait_send()
    send(GROUPS - 1)
    out = pltpu.make_async_copy(comp, comp_ref, local.at[7])
    out.start()
    pltpu.make_async_copy(tile.at[:, 0], o_ref.at[me], local.at[6]).wait()
    out.wait()
    others = o_ref.at[0:devices - 1]
    pltpu.make_async_remote_copy(
        src_ref=others, dst_ref=others, send_sem=sent.at[1], recv_sem=got_sem.at[0],
        device_id={"pix": peers[1]}, device_id_type=MESH,
    ).wait()


def spectrum_kernel(got, table, comp, o_ref, out_ref, order, out, outs):
    devices, columns = got.shape[0], got.shape[3]
    local_rows = out.shape[1]
    parts = outs.shape[0] - 1
    size = devices // parts

    def copy_out(n):
        at = pl.ds(n * size * columns, size * columns)
        return pltpu.make_async_copy(out.at[:, :, at], o_ref.at[:, :, at], outs.at[n])

    for c in range(2):
        for g in range(GROUPS):
            order[c, pl.ds(g, SUB, stride=GROUPS), :] = comp[c, g]
    last = pltpu.make_async_copy(order, out_ref, outs.at[parts])
    last.start()
    for n in range(parts):
        for m in range(0, size, 2):
            at = n * size + m
            both = jnp.concatenate(
                [got[at].reshape(2 * ROWS, columns), got[at + 1].reshape(2 * ROWS, columns)], axis=1
            )
            value = jnp.dot(
                table[...], jnp.concatenate([both, both], axis=0), preferred_element_type=jnp.float32
            )
            for c in range(2):
                out[c, :, at * columns:(at + 2) * columns] = value[c * local_rows:(c + 1) * local_rows]
        copy_out(n).start()
    for n in range(parts):
        copy_out(n).wait()
    last.wait()


def on_device(slcs, ref_date):
    devices = lax.axis_size("pix")
    local_rows, strip_columns = slcs.shape[1], slcs.shape[2]
    columns = strip_columns // devices
    per_date = ROWS // local_rows

    anywhere = pl.BlockSpec(memory_space=pl.ANY)
    hbm = pl.BlockSpec(memory_space=pltpu.HBM)
    vmem = pl.BlockSpec(memory_space=pltpu.VMEM)
    both, pick, order = window_weights(columns), pick_weights(columns), order_weights(local_rows)
    mask = block_masks()
    table = dct_weights(local_rows)
    f32, bf16 = jnp.float32, jnp.bfloat16
    phases, compressed = pl.pallas_call(
        functools.partial(link_kernel, devices),
        out_shape=(
            jax.ShapeDtypeStruct((devices, GROUPS, 2 * SUB, columns), bf16),
            jax.ShapeDtypeStruct((2, GROUPS, SUB, columns), f32),
        ),
        in_specs=[pl.BlockSpec(memory_space=pltpu.SMEM)] + [hbm] * 5,
        out_specs=(anywhere, anywhere),
        scratch_shapes=[
            pltpu.VMEM((2 * local_rows, strip_columns + 2 * columns), bf16),
            pltpu.VMEM((devices, 2 * local_rows, columns), bf16),
            pltpu.VMEM((devices, EDGE // 2, 2, LANES), bf16),
            pltpu.VMEM((devices, EDGE // 2, 2, LANES), bf16),
            pltpu.VMEM((DATES // PACK, 2, ROWS, LANES), f32),
            pltpu.VMEM((BATCH, 2, ROWS, LANES), f32),
            pltpu.VMEM(both.shape, bf16),
            pltpu.VMEM(pick.shape, bf16),
            pltpu.VMEM(order.shape, bf16),
            pltpu.VMEM(mask.shape, f32),
            pltpu.VMEM((BATCH, 2, ROWS, columns), f32),
            pltpu.VMEM((DATES, 2, ROWS, columns), f32),
            pltpu.VMEM((2 * BATCH * CHUNK * ROWS, columns), f32),
            pltpu.VMEM((GROUPS, SUB, columns), f32),
            pltpu.VMEM((GROUPS, DATES, DATES, 3, SUB, columns), f32),
            pltpu.VMEM((2, DATES, 3, SUB, columns), f32),
            pltpu.VMEM((GROUPS, DATES, 2 * SUB, columns), bf16),
            pltpu.VMEM((2, GROUPS, SUB, columns), f32),
            pltpu.SemaphoreType.DMA((8,)),
            pltpu.SemaphoreType.DMA((3,)),
            pltpu.SemaphoreType.DMA((devices,)),
            pltpu.SemaphoreType.DMA((devices,)),
            pltpu.SemaphoreType.DMA((1,)),
        ],
        compiler_params=pltpu.CompilerParams(
            collective_id=0, has_side_effects=True, vmem_limit_bytes=LINK_VMEM
        ),
        name="link",
    )(
        ref_date,
        *(
            pltpu.with_memory_space_constraint(value, pltpu.HBM)
            for value in (slcs.reshape(2 * local_rows, strip_columns), both, pick, order, mask)
        ),
    )

    if per_date > 1:
        table = lax.dynamic_index_in_dim(table, lax.rem(lax.axis_index("pix"), per_date), 0, False)
    else:
        table = table[0]
    parts = 4
    return pl.pallas_call(
        spectrum_kernel,
        out_shape=(
            jax.ShapeDtypeStruct((2, local_rows, strip_columns), f32),
            jax.ShapeDtypeStruct((2, ROWS, columns), f32),
        ),
        in_specs=[vmem] * 3,
        out_specs=(hbm, hbm),
        scratch_shapes=[
            pltpu.VMEM((2, ROWS, columns), f32),
            pltpu.VMEM((2, local_rows, strip_columns), f32),
            pltpu.SemaphoreType.DMA((parts + 1,)),
        ],
        compiler_params=pltpu.CompilerParams(vmem_limit_bytes=SPECTRUM_VMEM),
        name="spectrum",
    )(phases, table, compressed)


def solution(mesh):
    return jax.shard_map(
        on_device,
        mesh=mesh,
        in_specs=(P(None, ("grp", "pix"), None), P("grp")),
        out_specs=(P(None, ("grp", "pix"), None), P(None, None, ("grp", "pix"))),
        check_vma=False,
    )
```

```python
import functools
import math

import jax
import jax.numpy as jnp
import numpy as np
from jax import lax
from jax.experimental import pallas as pl
from jax.experimental.pallas import tpu as pltpu
from jax.sharding import PartitionSpec as P

DATES = 16
ROWS = 64
HALF_X = 5
HALF_Y = 2
POWER_ITERS = 6
LOADING = 0.25

LANES = 128
SUB = 8
GROUPS = ROWS // SUB
HALO = 16
EDGE = 2 * HALF_X
PACK = LANES // HALO
CHUNK = 8
BATCH = 2
FIRST = 8
SPAN = 8
SCALE = 2.0 ** -6
LINK_VMEM = 40 * 1024 * 1024
SPECTRUM_VMEM = 12 * 1024 * 1024
MESH = pl.DeviceIdType.MESH


def window_weights(columns):
    target = np.arange(columns)[None, :]
    band = np.abs(np.arange(columns)[:, None] - target) <= HALF_X
    outside = np.concatenate([np.arange(-HALF_X, 0), columns + np.arange(HALF_X)])
    halo = np.zeros((HALO, columns), np.float32)
    halo[: 2 * HALF_X] = np.abs(outside[:, None] - target) <= HALF_X
    both = np.concatenate([band.astype(np.float32), np.tile(halo, (PACK, 1))], axis=0)
    return jnp.asarray(both * SCALE, jnp.bfloat16)


def pick_weights(columns):
    pick = np.zeros((HALO, 2 * columns), np.float32)
    for h in range(HALF_X):
        pick[h, columns - HALF_X + h] = 1.0
        pick[HALF_X + h, columns + h] = 1.0
    return jnp.asarray(pick, jnp.bfloat16)


def order_weights(local_rows):
    per_date = ROWS // local_rows
    order = np.zeros((2, GROUPS, SUB, per_date, LANES), np.float32)
    for c in range(2):
        for line in range(ROWS):
            q, r = divmod(line, local_rows)
            order[c, line % GROUPS, line // GROUPS, q, c * local_rows + r] = 1.0
    return jnp.asarray(order.reshape(2 * ROWS, per_date * LANES), jnp.bfloat16)


def block_masks():
    block = np.arange(PACK)[:, None, None] == (np.arange(LANES) // HALO)[None, None, :]
    return jnp.asarray(np.broadcast_to(block, (PACK, 2 * SUB, LANES)), jnp.float32)


def dct_weights(local_rows):
    frequency = np.arange(ROWS, dtype=np.float64)[:, None]
    position = np.arange(ROWS, dtype=np.float64)[None, :]
    weight = np.where(frequency == 0, math.sqrt(1.0 / ROWS), math.sqrt(2.0 / ROWS))
    table = weight * np.cos(np.pi * (2.0 * position + 1.0) * frequency / (2.0 * ROWS))
    table = table.reshape(ROWS // local_rows, local_rows, SUB, GROUPS).transpose(0, 1, 3, 2)
    big = np.zeros((ROWS // local_rows, 2, local_rows, GROUPS, 2, SUB), np.float32)
    for c in range(2):
        big[:, c, :, :, c] = table
    big = big.reshape(ROWS // local_rows, 2 * local_rows, 2 * ROWS)
    high = big.astype(jnp.bfloat16)
    low = (big - high.astype(np.float32)).astype(jnp.bfloat16)
    return jnp.asarray(np.concatenate([high, low], axis=2))


def pair_products(one, two):
    real = one[0] * two[0] + one[1] * two[1]
    imag = one[1] * two[0] - one[0] * two[1]
    return real, imag


def tall_of(value, rows):
    return jnp.concatenate([value] * (rows // value.shape[0]), axis=0)


def flips(a, size):
    out, bit = [], 1
    while bit < size:
        out.append(bit - 2 * bit * ((a // bit) % 2))
        bit *= 2
    return out


def flipped(a, deltas, b):
    for n, delta in enumerate(deltas):
        if isinstance(b, int):
            a = a + delta if (b >> n) & 1 else a
        else:
            a = a + delta * ((b // (1 << n)) % 2)
    return a


def link_kernel(devices, ref_ref, x_ref, both_ref, pick_ref, order_ref, mask_ref,
                o_ref, comp_ref,
                xs, win, hsend, hwin, edge, wide, both, pick, order, mask,
                stage, zb, summed, spare, load, cov, vec, tile, comp,
                local, sent, rsem, hsem, got_sem):
    columns = win.shape[2]
    height = x_ref.shape[0]
    local_rows = height // 2
    strip_columns = x_ref.shape[1]
    per_date = ROWS // local_rows
    me = lax.axis_index("pix")
    my_date = me // per_date
    turns = flips(me, devices)
    date_turns = turns[(per_date - 1).bit_length():]
    peers = [flipped(me, turns, off) for off in range(devices)]
    bf16, f32 = jnp.bfloat16, jnp.float32

    barrier = pltpu.get_barrier_semaphore()
    for peer in peers[1:]:
        pl.semaphore_signal(barrier, inc=1, device_id={"pix": peer}, device_id_type=MESH)

    def block(n):
        return x_ref.at[:, pl.ds(pl.multiple_of(n * columns, columns), columns)]

    loads = [
        pltpu.make_async_copy(src, dst, local.at[n])
        for n, (src, dst) in enumerate((
            (x_ref, xs.at[:, columns:columns + strip_columns]),
            (pick_ref, pick), (block(me), win.at[me]), (both_ref, both), (order_ref, order),
            (mask_ref, mask),
        ))
    ]
    for copy in loads:
        copy.start()

    def main_copy(off, peer):
        return pltpu.make_async_remote_copy(
            src_ref=block(peer), dst_ref=win.at[me], send_sem=sent.at[0],
            recv_sem=rsem.at[off], device_id={"pix": peer}, device_id_type=MESH,
        )

    def halo_copy(off, peer):
        return pltpu.make_async_remote_copy(
            src_ref=hsend.at[peer], dst_ref=hwin.at[me], send_sem=sent.at[2],
            recv_sem=hsem.at[off], device_id={"pix": peer}, device_id_type=MESH,
        )

    queue = list(range(1, devices))
    first, later = queue[:FIRST], queue[FIRST:]
    halos = [halo_copy(off, peers[off]) for off in queue]
    mains = {off: main_copy(off, peers[off]) for off in range(1, devices)}

    pl.semaphore_wait(barrier, devices - 1)
    for off in first:
        mains[off].start()

    margin = jnp.zeros((height, columns), bf16)
    xs[:, 0:columns] = margin
    xs[:, columns + strip_columns:2 * columns + strip_columns] = margin
    loads[0].wait()
    loads[1].wait()

    blocks = min(devices, 16)

    def cut_halos(n, carry):
        for q in range(blocks):
            at = (n * blocks + q) * columns
            left = xs[:, pl.ds(pl.multiple_of(at, columns), columns)]
            right = xs[:, pl.ds(pl.multiple_of(at + 2 * columns, columns), columns)]
            near = jnp.concatenate([left, right], axis=1)
            if height < LANES:
                fill = jnp.zeros((LANES - height, 2 * columns), bf16)
                near = jnp.concatenate([near, fill], axis=0)
            got = lax.dot_general(
                pick[...], near, (((1,), (1,)), ((), ())), preferred_element_type=f32
            )
            for r in range(EDGE // 2):
                hsend[n * blocks + q, r] = got[2 * r:2 * r + 2].astype(bf16)
        return carry

    lax.fori_loop(0, devices // blocks, cut_halos, 0)
    hwin[me] = hsend[me]
    for c in halos:
        c.start()
    for off in later:
        mains[off].start()

    first_column = me * columns
    sub = lax.broadcasted_iota(jnp.int32, (SUB, columns), 0)
    lane = lax.broadcasted_iota(jnp.int32, (SUB, columns), 1) + first_column
    across = jnp.minimum(lane + HALF_X, strip_columns - 1) - jnp.maximum(lane - HALF_X, 0) + 1
    for g in range(GROUPS):
        line = sub * GROUPS + g
        along = jnp.minimum(line + HALF_Y, ROWS - 1) - jnp.maximum(line - HALF_Y, 0) + 1
        load[g] = (along * across).astype(f32) * (LOADING * SCALE)
    edge[...] = jnp.zeros_like(edge)
    for copy in loads[2:]:
        copy.wait()

    def tall(value):
        return tall_of(value, ROWS)

    def window_sums(plane):
        rows = [plane[g * SUB:(g + 1) * SUB] for g in range(GROUPS)]
        before = [jnp.where(sub == 0, 0.0, pltpu.roll(x, 1, 0)) for x in rows[-HALF_Y:]]
        after = [jnp.where(sub == SUB - 1, 0.0, pltpu.roll(x, SUB - 1, 0)) for x in rows[:HALF_Y]]
        ext = before + rows + after
        two = [ext[2 * k] + ext[2 * k + 1] for k in range(GROUPS // 2 + 2)]
        four = [two[k] + two[k + 1] for k in range(GROUPS // 2 + 1)]
        out = []
        for k in range(GROUPS // 2):
            out.append(four[k] + ext[2 * k + 4])
            out.append(ext[2 * k + 1] + four[k + 1])
        return out

    def finish(held, b, n):
        for d in range(BATCH):
            p = b * BATCH + d
            for q in range(CHUNK):
                first_row = (d * CHUNK + q) * 2 * ROWS
                sums = [
                    window_sums(held[first_row + part * ROWS:first_row + (part + 1) * ROWS])
                    for part in range(2)
                ]
                for g in range(GROUPS):
                    real, imag = sums[0][g], sums[1][g]
                    cov[g, p, n * CHUNK + q, 0] = real
                    cov[g, p, n * CHUNK + q, 1] = real + imag
                    cov[g, p, n * CHUNK + q, 2] = imag - real

    def diagonal(b):
        for g in range(GROUPS):
            more = load[g]
            for d in range(BATCH):
                p = b * BATCH + d
                cov[g, p, p, 0] = cov[g, p, p, 0] + more

    def begin(held, b, n):
        half = (n * CHUNK) // PACK
        planes = []
        beside = edge[half, 0].astype(bf16), edge[half, 1].astype(bf16)
        for d in range(BATCH):
            p = b * BATCH + d
            one = zb[p, 0].astype(bf16), zb[p, 1].astype(bf16)
            margins = pair_products((wide[d, 0].astype(bf16), wide[d, 1].astype(bf16)), beside)
            for q in range(CHUNK):
                k = n * CHUNK + q
                two = zb[k, 0].astype(bf16), zb[k, 1].astype(bf16)
                keep = tall(mask[k - half * PACK].astype(bf16))
                for value, margin in zip(pair_products(one, two), margins):
                    planes.append(jnp.concatenate([value, margin * keep], axis=1))
        held[...] = jnp.dot(
            jnp.concatenate(planes, axis=0), both[...], preferred_element_type=f32
        )

    def rows_of(ref, source):
        rows = [ref[source, r].astype(f32) for r in range(EDGE // 2)]
        return jnp.concatenate(rows + [jnp.zeros((HALO - EDGE, LANES), f32)], axis=0).astype(bf16)

    def covariances(chunks, b, prev):
        for n in range(BATCH * per_date):
            off = b * (BATCH * per_date) + n
            source = flipped(me, turns, off)

            @pl.when(off != 0)
            def _():
                pltpu.make_async_remote_copy(
                    src_ref=hwin.at[source], dst_ref=hwin.at[source], send_sem=sent.at[2],
                    recv_sem=hsem.at[off], device_id={"pix": source}, device_id_type=MESH,
                ).wait_recv()
                pltpu.make_async_remote_copy(
                    src_ref=win.at[source], dst_ref=win.at[source], send_sem=sent.at[0],
                    recv_sem=rsem.at[off], device_id={"pix": source}, device_id_type=MESH,
                ).wait_recv()

        for d in range(BATCH):
            p = b * BATCH + d
            date = flipped(my_date, date_turns, p)
            sources = [date * per_date + q for q in range(per_date)]
            margin = jnp.concatenate(
                [tall_of(rows_of(hwin, source), LANES) for source in sources], axis=1
            )
            got = lax.dot_general(
                order[...], margin, (((1,), (1,)), ((), ())), preferred_element_type=f32
            )
            keep = tall(mask[lax.rem(p, PACK)])
            half = p // PACK
            for c in range(2):
                part = got[c * ROWS:(c + 1) * ROWS]
                wide[d, c] = part
                edge[half, c] = edge[half, c] + part * keep
            for q, source in enumerate(sources):
                for c in range(2):
                    stage[d, c, q * local_rows:(q + 1) * local_rows] = win[
                        source, c * local_rows:(c + 1) * local_rows
                    ].astype(f32)
            for c in range(2):
                for g in range(GROUPS):
                    zb[p, c, g * SUB:(g + 1) * SUB] = stage[d, c, pl.ds(g, SUB, stride=GROUPS), :]

        for n in range(chunks - 1):
            begin(spare, b, n)
        finish(summed, prev, prev * BATCH // CHUNK)
        diagonal(prev)
        begin(summed, b, chunks - 1)
        for n in range(chunks - 1):
            finish(spare, b, n)
        return b

    middle = CHUNK // BATCH
    last = lax.fori_loop(0, middle, functools.partial(covariances, 1), jnp.int32(0))
    last = lax.fori_loop(middle, 2 * middle, functools.partial(covariances, 2), last)
    finish(summed, last, 1)
    diagonal(last)

    ref = flipped(my_date, date_turns, ref_ref[0])

    def send(g):
        for off in queue:
            pltpu.make_async_remote_copy(
                src_ref=tile.at[g, off // per_date], dst_ref=o_ref.at[me, g],
                send_sem=sent.at[1], recv_sem=got_sem.at[0],
                device_id={"pix": peers[off]}, device_id_type=MESH,
            ).start()
        pltpu.make_async_copy(tile.at[g, 0], o_ref.at[me, g], local.at[6]).start()

    column = [
        (
            jnp.maximum(ref, i), jnp.minimum(ref, i),
            jnp.where(ref == i, 0.0, jnp.where(ref < i, 0.5, -0.5)),
        )
        for i in range(DATES)
    ]

    def solve(g, carry):
        for i, (one, two, sign) in enumerate(column):
            real = cov[g, one, two, 0]
            imag = (cov[g, one, two, 1] + cov[g, one, two, 2]) * sign
            vec[0, i, 0] = real
            vec[0, i, 1] = imag
            vec[0, i, 2] = real + imag

        @pl.when(g > 0)
        def _():
            send(g - 1)

        def step(t):
            src = t % 2
            for base in range(0, DATES, SPAN):
                acc = [[None] * 3 for _ in range(SPAN)]
                for j in range(DATES):
                    vr, vi, vs = vec[src, j, 0], vec[src, j, 1], vec[src, j, 2]
                    for q in range(SPAN):
                        i = base + q
                        one, two = max(i, j), min(i, j)
                        cr = cov[g, one, two, 0]
                        if i == j:
                            terms, minus = (None, cr * vr, cr * vi), (False, True, False)
                        elif i > j:
                            terms = (cr * vs, cov[g, i, j, 1] * vi, cov[g, i, j, 2] * vr)
                            minus = (False, False, False)
                        else:
                            terms = (cr * vs, cov[g, j, i, 2] * vi, cov[g, j, i, 1] * vr)
                            minus = (False, True, True)
                        for n in range(3):
                            if terms[n] is None:
                                continue
                            if acc[q][n] is None:
                                acc[q][n] = -terms[n] if minus[n] else terms[n]
                            elif minus[n]:
                                acc[q][n] = acc[q][n] - terms[n]
                            else:
                                acc[q][n] = acc[q][n] + terms[n]
                for q in range(SPAN):
                    real, imag = acc[q][0] - acc[q][1], acc[q][0] + acc[q][2]
                    vec[1 - src, base + q, 0] = real
                    vec[1 - src, base + q, 1] = imag
                    vec[1 - src, base + q, 2] = real + imag

        for t in range(POWER_ITERS - 1):
            step(t)
        last = (POWER_ITERS - 1) % 2
        total = jnp.zeros((SUB, columns), f32)
        for k in range(DATES):
            vr, vi = vec[last, k, 0], vec[last, k, 1]
            total = total + (vr * vr + vi * vi)
        scale = DATES / total
        rr, ri = vec[last, ref, 0] * scale, vec[last, ref, 1] * scale
        comp_r = jnp.zeros_like(total)
        comp_i = jnp.zeros_like(total)
        at = pl.ds(pl.multiple_of(g * SUB, SUB), SUB)
        for k in range(DATES):
            vr, vi = vec[last, k, 0], vec[last, k, 1]
            lr = vr * rr + vi * ri
            li = vi * rr - vr * ri
            zr, zi = zb[k, 0, at], zb[k, 1, at]
            comp_r = comp_r + (lr * zr + li * zi)
            comp_i = comp_i + (lr * zi - li * zr)
            tile[g, k] = jnp.concatenate([lr, li], axis=0).astype(bf16)
        comp[0, g] = comp_r * (1.0 / math.sqrt(DATES))
        comp[1, g] = comp_i * (1.0 / math.sqrt(DATES))
        return carry

    lax.fori_loop(0, GROUPS, solve, 0)
    pltpu.make_async_remote_copy(
        src_ref=win.at[0:devices - 1], dst_ref=win.at[0:devices - 1], send_sem=sent.at[0],
        recv_sem=rsem.at[0], device_id={"pix": peers[1]}, device_id_type=MESH,
    ).wait_send()
    pltpu.make_async_remote_copy(
        src_ref=hwin.at[0:devices - 1], dst_ref=hwin.at[0:devices - 1], send_sem=sent.at[2],
        recv_sem=hsem.at[0], device_id={"pix": peers[1]}, device_id_type=MESH,
    ).wait_send()
    send(GROUPS - 1)
    out = pltpu.make_async_copy(comp, comp_ref, local.at[7])
    out.start()
    pltpu.make_async_copy(tile.at[:, 0], o_ref.at[me], local.at[6]).wait()
    out.wait()
    others = o_ref.at[0:devices - 1]
    pltpu.make_async_remote_copy(
        src_ref=others, dst_ref=others, send_sem=sent.at[1], recv_sem=got_sem.at[0],
        device_id={"pix": peers[1]}, device_id_type=MESH,
    ).wait()


def spectrum_kernel(got, table, comp, o_ref, out_ref, order, out, outs):
    devices, columns = got.shape[0], got.shape[3]
    local_rows = out.shape[1]
    parts = outs.shape[0] - 1
    size = devices // parts

    def copy_out(n):
        at = pl.ds(n * size * columns, size * columns)
        return pltpu.make_async_copy(out.at[:, :, at], o_ref.at[:, :, at], outs.at[n])

    for c in range(2):
        for g in range(GROUPS):
            order[c, pl.ds(g, SUB, stride=GROUPS), :] = comp[c, g]
    last = pltpu.make_async_copy(order, out_ref, outs.at[parts])
    last.start()
    for n in range(parts):
        for m in range(0, size, 2):
            at = n * size + m
            both = jnp.concatenate(
                [got[at].reshape(2 * ROWS, columns), got[at + 1].reshape(2 * ROWS, columns)], axis=1
            )
            value = jnp.dot(
                table[...], jnp.concatenate([both, both], axis=0), preferred_element_type=jnp.float32
            )
            for c in range(2):
                out[c, :, at * columns:(at + 2) * columns] = value[c * local_rows:(c + 1) * local_rows]
        copy_out(n).start()
    for n in range(parts):
        copy_out(n).wait()
    last.wait()


def on_device(slcs, ref_date):
    devices = lax.axis_size("pix")
    local_rows, strip_columns = slcs.shape[1], slcs.shape[2]
    columns = strip_columns // devices
    per_date = ROWS // local_rows

    anywhere = pl.BlockSpec(memory_space=pl.ANY)
    hbm = pl.BlockSpec(memory_space=pltpu.HBM)
    vmem = pl.BlockSpec(memory_space=pltpu.VMEM)
    both, pick, order = window_weights(columns), pick_weights(columns), order_weights(local_rows)
    mask = block_masks()
    table = dct_weights(local_rows)
    f32, bf16 = jnp.float32, jnp.bfloat16
    phases, compressed = pl.pallas_call(
        functools.partial(link_kernel, devices),
        out_shape=(
            jax.ShapeDtypeStruct((devices, GROUPS, 2 * SUB, columns), bf16),
            jax.ShapeDtypeStruct((2, GROUPS, SUB, columns), f32),
        ),
        in_specs=[pl.BlockSpec(memory_space=pltpu.SMEM)] + [hbm] * 5,
        out_specs=(anywhere, anywhere),
        scratch_shapes=[
            pltpu.VMEM((2 * local_rows, strip_columns + 2 * columns), bf16),
            pltpu.VMEM((devices, 2 * local_rows, columns), bf16),
            pltpu.VMEM((devices, EDGE // 2, 2, LANES), bf16),
            pltpu.VMEM((devices, EDGE // 2, 2, LANES), bf16),
            pltpu.VMEM((DATES // PACK, 2, ROWS, LANES), f32),
            pltpu.VMEM((BATCH, 2, ROWS, LANES), f32),
            pltpu.VMEM(both.shape, bf16),
            pltpu.VMEM(pick.shape, bf16),
            pltpu.VMEM(order.shape, bf16),
            pltpu.VMEM(mask.shape, f32),
            pltpu.VMEM((BATCH, 2, ROWS, columns), f32),
            pltpu.VMEM((DATES, 2, ROWS, columns), f32),
            pltpu.VMEM((2 * BATCH * CHUNK * ROWS, columns), f32),
            pltpu.VMEM((2 * BATCH * CHUNK * ROWS, columns), f32),
            pltpu.VMEM((GROUPS, SUB, columns), f32),
            pltpu.VMEM((GROUPS, DATES, DATES, 3, SUB, columns), f32),
            pltpu.VMEM((2, DATES, 3, SUB, columns), f32),
            pltpu.VMEM((GROUPS, DATES, 2 * SUB, columns), bf16),
            pltpu.VMEM((2, GROUPS, SUB, columns), f32),
            pltpu.SemaphoreType.DMA((8,)),
            pltpu.SemaphoreType.DMA((3,)),
            pltpu.SemaphoreType.DMA((devices,)),
            pltpu.SemaphoreType.DMA((devices,)),
            pltpu.SemaphoreType.DMA((1,)),
        ],
        compiler_params=pltpu.CompilerParams(
            collective_id=0, has_side_effects=True, vmem_limit_bytes=LINK_VMEM
        ),
        name="link",
    )(
        ref_date,
        *(
            pltpu.with_memory_space_constraint(value, pltpu.HBM)
            for value in (slcs.reshape(2 * local_rows, strip_columns), both, pick, order, mask)
        ),
    )

    if per_date > 1:
        table = lax.dynamic_index_in_dim(table, lax.rem(lax.axis_index("pix"), per_date), 0, False)
    else:
        table = table[0]
    parts = 4
    return pl.pallas_call(
        spectrum_kernel,
        out_shape=(
            jax.ShapeDtypeStruct((2, local_rows, strip_columns), f32),
            jax.ShapeDtypeStruct((2, ROWS, columns), f32),
        ),
        in_specs=[vmem] * 3,
        out_specs=(hbm, hbm),
        scratch_shapes=[
            pltpu.VMEM((2, ROWS, columns), f32),
            pltpu.VMEM((2, local_rows, strip_columns), f32),
            pltpu.SemaphoreType.DMA((parts + 1,)),
        ],
        compiler_params=pltpu.CompilerParams(vmem_limit_bytes=SPECTRUM_VMEM),
        name="spectrum",
    )(phases, table, compressed)


def solution(mesh):
    return jax.shard_map(
        on_device,
        mesh=mesh,
        in_specs=(P(None, ("grp", "pix"), None), P("grp")),
        out_specs=(P(None, ("grp", "pix"), None), P(None, None, ("grp", "pix"))),
        check_vma=False,
    )
```
